32 devices in a mesh: gx: 4 (over z), gy: 2 (over x), gz: 4 (over y, core).
Axes of the slice: x: 2, y: 2, z: 4, core: 2. Of those that a mesh axis runs over, the one named last changes fastest.
Arguments:
- old_slots: bfloat16 [4, 2, 32, 4096], P('gx', 'gy', 'gz'), may hold values from -6 to 6
- old_ids: int32 [4, 2, 32], P('gx', 'gy', 'gz'), may hold values from -1 to 31, as said below
- old_owner: int32 [4, 2, 32], P('gx', 'gy'), may hold values from 0 to 3, as said below
- coefficient: float32 [64, 32, 512], P('gx', 'gy', 'gz'), may hold values from 0.2 to 5
Outputs:
- solution: float32 [64, 32, 512], P('gx', 'gy', 'gz')
The draws below stay inside these ranges and needn't reach their ends.
Inputs may be any that keep to these rules, and one draw needn't show every extreme that they name: old_owner[a, c, b] is the index along gz of the device that held box b of box column (a, c) before the move; no device holds more than 8 boxes of a column and some device holds exactly 8; no device holds more than 2 of the 8 boxes with one value of b // 8, and that bound is reached. old_ids[a, c, g * 8 + q] is the box held in slot q of device g of box column (a, c), or -1 for an empty slot; it agrees with old_owner and each box stands in exactly one slot.
All inputs are finite; a program needn't handle non-finite values.
Results may differ from the reference program's by a relative error of at most 0.0003.
Values may be sent and summed in bfloat16 or wider, within the bound.
No kernel may reach another device: no remote copies, remote signals or barrier semaphores. Data moves between devices by JAX's collectives and lax.ppermute only.
A program may use at most 64 MiB of HBM per device.

```python
import math
import jax
import jax.numpy as jnp
from jax import lax

BOX = 16
NB = 8
SWEEPS = 2
CAP = 8
NX = 64
NY = 32
NZ = 512
N_GX = 4
N_GY = 2
N_GZ = 4


def column_maps(column_key):
    groups = N_GZ
    halves = NB // 2
    pair_count = groups * halves
    subkeys = jax.random.split(column_key, 5)
    labels = jnp.arange(groups, dtype=jnp.int32)
    if NB <= groups:
        counts = jnp.where(labels < groups // 4, 2 * halves, jnp.where(labels < groups // 2, halves, halves // 2)).astype(jnp.int32)
    else:
        counts = jnp.full((groups,), halves, jnp.int32)
    ending = jnp.cumsum(counts).astype(jnp.int32)
    items = jnp.arange(pair_count, dtype=jnp.int32)
    sorted_owner = jnp.sum((items[:, None] >= ending[None, :]).astype(jnp.int32), axis=1)
    relabel = jax.random.permutation(subkeys[0], groups).astype(jnp.int32)
    item_owner = relabel[sorted_owner]
    columns = jax.random.permutation(subkeys[1], groups).astype(jnp.int32)
    target = columns[items % groups]
    levels = items // groups
    placing = jax.vmap(lambda single: jax.random.permutation(single, NB).astype(jnp.int32))(jax.random.split(subkeys[2], groups))
    first_box = target * NB + placing[target, 2 * levels]
    second_box = target * NB + placing[target, 2 * levels + 1]
    box_count = groups * NB
    owners = jnp.zeros((box_count,), jnp.int32).at[first_box].set(item_owner).at[second_box].set(item_owner)
    priority = jax.random.permutation(subkeys[3], box_count).astype(jnp.int32)
    sharing = owners[:, None] == owners[None, :]
    ranking = jnp.sum((sharing & (priority[None, :] < priority[:, None])).astype(jnp.int32), axis=1)
    offsets = jax.random.randint(subkeys[4], (groups,), 0, CAP, dtype=jnp.int32)
    slot_index = (ranking + offsets[owners]) % CAP
    slot_ids = jnp.full((groups * CAP,), -1, jnp.int32).at[owners * CAP + slot_index].set(jnp.arange(box_count, dtype=jnp.int32))
    return (owners, slot_ids)


def all_columns(key):
    column_keys = jax.random.split(jax.random.fold_in(key, 31), N_GX * N_GY)
    return jax.vmap(column_maps)(column_keys)


def draw_old_owner(key, part):
    owners, slot_ids = all_columns(key)
    return owners.reshape(N_GX, N_GY, N_GZ * NB)


def draw_old_ids(key, part):
    owners, slot_ids = all_columns(key)
    return slot_ids.reshape(N_GX, N_GY, N_GZ * CAP)


def draw_old_slots(key, part):
    shape = (N_GX, N_GY, N_GZ * CAP, BOX ** 3)
    noise_key = jax.random.fold_in(jax.random.fold_in(key, 47), 0)
    return jnp.clip(jax.random.normal(noise_key, shape, jnp.float32), -6.0, 6.0).astype(jnp.bfloat16)


def level_of(own_key, extent, cuts, low, largest):
    gain, own = 1.0, jax.random.fold_in(own_key, 6)
    for axis_at, shards_of in cuts:
        draws = jnp.exp(jax.random.uniform(jax.random.fold_in(own, axis_at), (shards_of,), jnp.float32, low / len(cuts), largest / len(cuts)))
        gain = gain * jnp.repeat(draws, extent[axis_at] // shards_of).reshape([-1 if axis == axis_at else 1 for axis in range(len(extent))])
    return gain


def setup_inputs(seed: int = 0) -> dict:
    key_list = jax.random.split(jax.random.key(seed), 5)
    return {
        "old_slots": draw_old_slots(jax.random.fold_in(key_list[4], 71), 0),
        "old_ids": draw_old_ids(jax.random.fold_in(key_list[4], 71), 0),
        "old_owner": draw_old_owner(jax.random.fold_in(key_list[4], 71), 0),
        "coefficient": jnp.clip(jnp.exp(math.log(5.0) - 3.218876 * jax.random.uniform(key_list[3], (NX, NY, NZ), jnp.float32) ** level_of(key_list[3], (NX, NY, NZ), ((0, 4), (1, 2), (2, 4)), -0.2, 0.2)), 0.2, 5.0),
    }


def inner(padded):
    return padded[1:-1, 1:-1, 1:-1]


def operator_parts(padded):
    face_first = 0.5 * (padded[:-1, 1:-1, 1:-1] + padded[1:, 1:-1, 1:-1])
    face_second = 0.5 * (padded[1:-1, :-1, 1:-1] + padded[1:-1, 1:, 1:-1])
    face_third = 0.5 * (padded[1:-1, 1:-1, :-1] + padded[1:-1, 1:-1, 1:])
    diagonal = face_first[:-1] + face_first[1:] + face_second[:, :-1] + face_second[:, 1:] + face_third[:, :, :-1] + face_third[:, :, 1:]
    return face_first, face_second, face_third, diagonal


def neighbours(padded, stencil):
    face_first, face_second, face_third, diagonal = stencil
    summed = face_first[:-1] * padded[:-2, 1:-1, 1:-1] + face_first[1:] * padded[2:, 1:-1, 1:-1]
    summed = summed + face_second[:, :-1] * padded[1:-1, :-2, 1:-1] + face_second[:, 1:] * padded[1:-1, 2:, 1:-1]
    summed = summed + face_third[:, :, :-1] * padded[1:-1, 1:-1, :-2] + face_third[:, :, 1:] * padded[1:-1, 1:-1, 2:]
    return summed


def red_cells(shape, margin):
    index_first = lax.broadcasted_iota(jnp.int32, shape, 0)
    index_second = lax.broadcasted_iota(jnp.int32, shape, 1)
    index_third = lax.broadcasted_iota(jnp.int32, shape, 2)
    return (index_first + index_second + index_third + margin) % 2 == 0


def relax(padded, source, stencil, factor, chosen):
    fresh = (factor * source + neighbours(padded, stencil)) / stencil[3]
    return jnp.where(chosen, fresh, inner(padded))


def apply_operator(values, stencil, factor):
    return (stencil[3] * values - neighbours(jnp.pad(values, 1), stencil)) / factor


def smooth(values, source, stencil, factor):
    red_mask = red_cells(source.shape, 0)
    black_mask = jnp.logical_not(red_mask)
    for counter in range(SWEEPS):
        values = relax(jnp.pad(values, 1), source, stencil, factor, red_mask)
        values = relax(jnp.pad(values, 1), source, stencil, factor, black_mask)
    return values


def coarsen(values):
    extent_first, extent_second, extent_third = values.shape
    grouped = values.reshape(extent_first // 2, 2, extent_second // 2, 2, extent_third // 2, 2)
    return grouped.mean(axis=(1, 3, 5))


def refine(values):
    return jnp.repeat(jnp.repeat(jnp.repeat(values, 2, axis=0), 2, axis=1), 2, axis=2)


def bicgstab(rhs_low, stencil, factor):
    image_low = apply_operator(rhs_low, stencil, factor)
    alpha_step = jnp.sum(rhs_low * rhs_low) / jnp.sum(rhs_low * image_low)
    rest_low = rhs_low - alpha_step * image_low
    turned = apply_operator(rest_low, stencil, factor)
    omega_step = jnp.sum(turned * rest_low) / jnp.sum(turned * turned)
    return alpha_step * rhs_low + omega_step * rest_low


def move_boxes(old_slots, old_ids, old_owner):
    column_boxes = NB * N_GZ
    held = old_ids.reshape(N_GX, N_GY, N_GZ, CAP)
    owner_index = jnp.broadcast_to(old_owner[:, :, :, None], (N_GX, N_GY, column_boxes, CAP))
    owner_slots = jnp.take_along_axis(held, owner_index, axis=2)
    wanted = jnp.arange(column_boxes, dtype=jnp.int32)
    position = jnp.argmax(owner_slots == wanted[None, None, :, None], axis=3).astype(jnp.int32)
    global_slot = old_owner * CAP + position
    picked = jax.vmap(jax.vmap(lambda stacked, chosen_rows: stacked[chosen_rows]))(old_slots, global_slot)
    boxes = picked.reshape(N_GX, N_GY, column_boxes, BOX, BOX, BOX).transpose(0, 3, 1, 4, 2, 5)
    return boxes.reshape(N_GX * BOX, N_GY * BOX, column_boxes * BOX)


def reference(old_slots, old_ids, old_owner, coefficient):
    source_fine = move_boxes(old_slots, old_ids, old_owner).astype(jnp.float32)
    stencil_fine = operator_parts(jnp.pad(coefficient, 1))
    fine_values = smooth(jnp.zeros_like(source_fine), source_fine, stencil_fine, 1.0)
    residual_fine = source_fine - apply_operator(fine_values, stencil_fine, 1.0)
    coefficient_mid = coarsen(coefficient)
    stencil_mid = operator_parts(jnp.pad(coefficient_mid, 1))
    source_mid = coarsen(residual_fine)
    middle_values = smooth(jnp.zeros_like(source_mid), source_mid, stencil_mid, 4.0)
    residual_mid = source_mid - apply_operator(middle_values, stencil_mid, 4.0)
    coefficient_low = coarsen(coefficient_mid)
    stencil_low = operator_parts(jnp.pad(coefficient_low, 1))
    bottom_values = bicgstab(coarsen(residual_mid), stencil_low, 16.0)
    middle_values = smooth(middle_values + refine(bottom_values), source_mid, stencil_mid, 4.0)
    return smooth(fine_values + refine(middle_values), source_fine, stencil_fine, 1.0)
```

```python
import jax
import jax.numpy as jnp
from jax import lax
from jax.experimental import pallas as pl
from jax.experimental.pallas import tpu as pltpu
from jax.sharding import PartitionSpec as P

BOX = 16
HALO = 8
LANES = 128
HIGH = lax.Precision.HIGHEST
F32 = jnp.float32
BF16 = jnp.bfloat16


def iota(shape, dim):
    return lax.broadcasted_iota(jnp.int32, shape, dim)


def exact_dot(left, right):
    return lax.dot_general(
        left, right, (((1,), (0,)), ((), ())), precision=HIGH, preferred_element_type=F32
    )


def even_rows(shape, dims):
    total = iota(shape, dims[0])
    for dim in dims[1:]:
        total = total + iota(shape, dim)
    return total % 2 == 0


def call(kernel, outs, scratch=(), **more):
    return pl.pallas_call(
        kernel,
        out_shape=outs,
        scratch_shapes=list(scratch),
        compiler_params=pltpu.CompilerParams(vmem_limit_bytes=48 * 1024 * 1024),
        **more,
    )


def shape_f32(*dims):
    return jax.ShapeDtypeStruct(dims, F32)


class Geometry:
    def __init__(self, sizes, block):
        self.gx, self.gy, self.gz = sizes
        self.bx, self.by, self.bz = block
        self.swap = self.gy == 2
        self.wx = self.bx + 2 * HALO
        self.wy = self.by + (HALO if self.swap else 2 * HALO)

    def own_y(self):
        if self.swap:
            return pl.multiple_of(lax.axis_index("gy") * HALO, HALO)
        return HALO

    def halo_y(self):
        if self.swap:
            return (pl.multiple_of((1 - lax.axis_index("gy")) * self.by, HALO),)
        return (0, HALO + self.by)


def neighbours_of(axis, count, step):
    if step > 0:
        return [(i, i + 1) for i in range(count - 1)]
    return [(i + 1, i) for i in range(count - 1)]


def pack_coefficient(geo, own, before, after):
    bx, by, bz = geo.bx, geo.by, geo.bz
    half = bz // 2

    def kernel(own_ref, before_ref, after_ref, out_ref, *sends):
        rows = bx * by
        lane = iota((rows, bz), 1)
        mine = own_ref[...].reshape(rows, bz)
        near = jnp.where(
            lane < half, after_ref[...].reshape(rows, bz), before_ref[...].reshape(rows, bz)
        )
        source = iota((bz, LANES), 0)
        target = iota((bz, LANES), 1)

        def pick(shift):
            low = (source == 2 * target + shift).astype(F32)
            high = (source == 2 * target + shift - bz).astype(F32)
            return exact_dot(mine, low) + exact_dot(near, high)

        even = pick(0).reshape(bx, by, LANES)
        odd = pick(1).reshape(bx, by, LANES)
        first = even_rows((bx, by, LANES), (0, 1))
        out_ref[0] = jnp.where(first, even, odd)
        out_ref[1] = jnp.where(first, odd, even)
        emit_sends(geo, out_ref, sends)

    return call(kernel, [shape_f32(2, bx, by, LANES)] + send_shapes(geo))(own, before, after)


def send_shapes(geo):
    one = shape_f32(2, geo.bx, HALO, LANES)
    return [one] if geo.swap else [one, one]


def emit_sends(geo, out_ref, sends):
    top = geo.by - HALO
    if geo.swap:
        start = pl.multiple_of((1 - lax.axis_index("gy")) * top, HALO)
        sends[0][...] = out_ref[:, :, pl.ds(start, HALO), :]
    else:
        sends[0][...] = out_ref[:, :, 0:HALO, :]
        sends[1][...] = out_ref[:, :, top : top + HALO, :]


def pack_source(geo, slots, cells):
    bx, by = geo.bx, geo.by
    count = slots.shape[0]
    tiles = cells // LANES
    boxes = 2 * geo.bz // BOX
    own_boxes = geo.bz // BOX
    per_tile = LANES // BOX
    pair = BOX // 2

    def kernel(slot_ref, out_ref, *rest):
        sends, ordered = rest[:-1], rest[-1]
        ids = slot_ref[:, cells : cells + LANES].astype(F32)
        place = iota((count, LANES), 1)
        wanted = jnp.where(place < own_boxes + own_boxes // 2, place, place - boxes)
        wanted = (wanted + lax.axis_index("gz") * own_boxes).astype(F32)
        chosen = jnp.where((ids == wanted) & (ids >= 0.0) & (place < boxes), 1.0, 0.0)
        chosen = chosen.T[0:boxes].astype(BF16)
        for tile in range(tiles):
            ordered[tile] = jnp.dot(
                chosen,
                slot_ref[:, tile * LANES : (tile + 1) * LANES],
                preferred_element_type=F32,
            )
        rows = tiles * per_tile
        keep = iota((tiles, per_tile, LANES), 2) // BOX == iota((tiles, per_tile, LANES), 1)
        inside = iota((LANES, 2 * LANES), 0) % BOX
        target = iota((LANES, 2 * LANES), 1)
        slot_of = jnp.where(
            inside % 2 == 0, inside // 2, inside // 2 + LANES
        )
        total = jnp.zeros((rows, 2 * LANES), F32)
        for box in range(boxes):
            line = jnp.broadcast_to(ordered[:, box : box + 1, :], (tiles, per_tile, LANES))
            line = jnp.where(keep, line, 0.0).reshape(rows, LANES).astype(BF16)
            spread = (target == slot_of + box * pair).astype(F32).astype(BF16)
            total = total + jnp.dot(line, spread, preferred_element_type=F32)
        even = total[:, 0:LANES].reshape(bx, by, LANES)
        odd = total[:, LANES:].reshape(bx, by, LANES)
        first = even_rows((bx, by, LANES), (0, 1))
        out_ref[0] = jnp.where(first, even, odd)
        out_ref[1] = jnp.where(first, odd, even)
        emit_sends(geo, out_ref, sends)

    return call(
        kernel,
        [shape_f32(2, bx, by, LANES)] + send_shapes(geo),
        [pltpu.VMEM((tiles, boxes, LANES), F32)],
    )(slots)


def exchange_y(geo, sends):
    if geo.swap:
        return (lax.ppermute(sends[0], "gy", [(0, 1), (1, 0)]),)
    low, high = sends
    return (
        lax.ppermute(high, "gy", neighbours_of("gy", geo.gy, 1)),
        lax.ppermute(low, "gy", neighbours_of("gy", geo.gy, -1)),
    )


def widen_y(geo, own, halos):
    half = geo.bx // 2

    def kernel(own_ref, *rest):
        halo_refs, outs = rest[:-2], rest[-2:]
        for part, out in enumerate(outs):
            span = slice(part * half, (part + 1) * half)
            out[:, :, pl.ds(geo.own_y(), geo.by), :] = own_ref[:, span]
            for halo, start in zip(halo_refs, geo.halo_y()):
                out[:, :, pl.ds(start, HALO), :] = halo[:, span]

    slab = shape_f32(2, half, geo.wy, LANES)
    return call(kernel, [slab, slab])(own, *halos)


def exchange_x(geo, low, high):
    return (
        lax.ppermute(high, "gx", neighbours_of("gx", geo.gx, 1)),
        lax.ppermute(low, "gx", neighbours_of("gx", geo.gx, -1)),
    )


PAD = 8


def fine_sum(geo, ref, row, near_low):
    rows = slice(PAD, PAD + geo.wy)
    here = ref[row, rows, :]
    total = ref[row - 1, rows, :] + ref[row + 1, rows, :] + here
    total = total + ref[row, PAD - 1 : PAD - 1 + geo.wy, :]
    total = total + ref[row, PAD + 1 : PAD + 1 + geo.wy, :]
    low = pltpu.roll(here, 1, 1)
    high = pltpu.roll(here, LANES - 1, 1)
    return total + jnp.where(near_low, low, high)


def fine_rows(geo, body):
    even = iota((geo.wy, LANES), 0) % 2 == 0
    odd = jnp.logical_not(even)

    def step(index, carry):
        body(2 * index + 1, 2 * index, even)
        body(2 * index + 2, 2 * index + 1, odd)
        return carry

    lax.fori_loop(0, geo.wx // 2, step, 0)


def fine_half(geo, colour, coeff, weight, source, values, scaled, extra=None):
    other = 1 - colour

    def body(row, cell, low):
        near_low = low if colour == 0 else jnp.logical_not(low)
        rows = slice(PAD, PAD + geo.wy)
        mine = coeff[colour][row, rows, :]
        summed = mine * fine_sum(geo, values[other], row, near_low)
        summed = summed + fine_sum(geo, scaled[other], row, near_low)
        fresh = weight[colour][cell] * (source[colour][cell] + summed)
        values[colour][row, rows, :] = fresh
        scaled[colour][row, rows, :] = mine * fresh

    fine_rows(geo, body)


def clear_pads(geo, ref):
    blank_row = jnp.zeros((geo.wy + 2 * PAD, LANES), F32)
    ref[0] = blank_row
    ref[geo.wx + 1] = blank_row
    edge = jnp.zeros((geo.wx + 2, PAD, LANES), F32)
    ref[:, 0:PAD, :] = edge
    ref[:, PAD + geo.wy : PAD + geo.wy + PAD, :] = edge


def fine_scratch(geo):
    return pltpu.VMEM((geo.wx + 2, geo.wy + 2 * PAD, LANES), F32)


def fine_before(geo, coefficient, source):
    half = geo.bx // 2
    wx, wy = geo.wx, geo.wy
    cx, cy = geo.bx // 2, geo.by // 2

    def kernel(*refs):
        coeff_in, source_in = refs[0:4], refs[4:8]
        coarse_ref, out_black, out_coeff, out_weight, out_source = refs[8:13]
        kr, kb, vr, vb, wr, wb, diag, resid = refs[13:]
        coeff, values, scaled = (kr, kb), (vr, vb), (wr, wb)
        rows = slice(PAD, PAD + wy)
        for ref in (kr, kb, vr, vb, wr, wb):
            clear_pads(geo, ref)
        start = 0
        for slab, slab_source in zip(coeff_in, source_in):
            depth = slab.shape[1]
            for colour in (0, 1):
                scaled_slab = 0.5 * slab[colour]
                coeff[colour][1 + start : 1 + start + depth, rows, :] = scaled_slab
                out_coeff[colour, start : start + depth] = scaled_slab
                out_source[colour, start : start + depth] = slab_source[colour]
            start += depth
        weight = (out_weight.at[0], out_weight.at[1])
        source_at = (out_source.at[0], out_source.at[1])

        def first_red(row, cell, low):
            mine = kr[row, rows, :]
            total = 6.0 * mine + fine_sum(geo, kb, row, low)
            inverse = jnp.where(mine > 0.0, 1.0 / total, 0.0)
            diag[cell] = total
            out_weight[0, cell] = inverse
            fresh = inverse * out_source[0, cell]
            vr[row, rows, :] = fresh
            wr[row, rows, :] = mine * fresh

        fine_rows(geo, first_red)

        def first_black(row, cell, low):
            high = jnp.logical_not(low)
            mine = kb[row, rows, :]
            total = 6.0 * mine + fine_sum(geo, kr, row, high)
            inverse = jnp.where(mine > 0.0, 1.0 / total, 0.0)
            out_weight[1, cell] = inverse

        fine_rows(geo, first_black)
        fine_half(geo, 1, coeff, weight, source_at, values, scaled)
        fine_half(geo, 0, coeff, weight, source_at, values, scaled)
        fine_half(geo, 1, coeff, weight, source_at, values, scaled)

        def residual(row, cell, low):
            mine = kr[row, rows, :]
            summed = mine * fine_sum(geo, vb, row, low) + fine_sum(geo, wb, row, low)
            resid[cell] = out_source[0, cell] + summed - diag[cell] * vr[row, rows, :]
            out_black[cell] = vb[row, rows, :]

        fine_rows(geo, residual)

        own = geo.own_y()
        for cell in range(cx):
            at = HALO + 2 * cell
            pair = resid[at] + resid[at + 1]
            diag[at] = pair
            mine = kr[at + 1, rows, :] + kr[at + 2, rows, :]
            mine = mine + kb[at + 1, rows, :] + kb[at + 2, rows, :]
            diag[at + 1] = mine
            for which, scale in ((0, 0.125), (1, 0.25)):
                low = diag[at + which, pl.ds(own, cy, 2), :]
                high = diag[at + which, pl.ds(own + 1, cy, 2), :]
                coarse_ref[which, cell] = scale * (low + high)

    window = shape_f32(wx, wy, LANES)
    both = shape_f32(2, wx, wy, LANES)
    return call(
        kernel,
        [shape_f32(2, cx, cy, LANES), window, both, both, both],
        [fine_scratch(geo)] * 6 + [pltpu.VMEM((wx, wy, LANES), F32)] * 2,
    )(*coefficient, *source)


def mid_sum(my, ref, row):
    rows = slice(PAD, PAD + my)
    here = ref[row, rows, :]
    total = ref[row - 1, rows, :] + ref[row + 1, rows, :]
    total = total + ref[row, PAD - 1 : PAD - 1 + my, :]
    total = total + ref[row, PAD + 1 : PAD + 1 + my, :]
    return total + pltpu.roll(here, 1, 1) + pltpu.roll(here, LANES - 1, 1)


def mid_rows(mx, my, body):
    even = (iota((my, LANES), 0) + iota((my, LANES), 1)) % 2 == 0
    odd = jnp.logical_not(even)

    def step(index, carry):
        body(2 * index + 1, 2 * index, even)
        body(2 * index + 2, 2 * index + 1, odd)
        return carry

    lax.fori_loop(0, mx // 2, step, 0)


def mid_half(mx, my, colour, coeff, weight, source, values, scaled):
    rows = slice(PAD, PAD + my)

    def body(row, cell, red):
        chosen = red if colour == 0 else jnp.logical_not(red)
        mine = coeff[row, rows, :]
        summed = mine * mid_sum(my, values, row) + mid_sum(my, scaled, row)
        fresh = weight[cell] * (source[cell] + summed)
        fresh = jnp.where(chosen, fresh, values[row, rows, :])
        values[row, rows, :] = fresh
        scaled[row, rows, :] = mine * fresh

    mid_rows(mx, my, body)


def clear_mid(mx, my, ref):
    ref[0] = jnp.zeros((my + 2 * PAD, LANES), F32)
    ref[mx + 1] = jnp.zeros((my + 2 * PAD, LANES), F32)
    edge = jnp.zeros((mx + 2, PAD, LANES), F32)
    ref[:, 0:PAD, :] = edge
    ref[:, PAD + my : PAD + my + PAD, :] = edge


def mid_before(geo, gathered):
    depth, my = gathered.shape[2], gathered.shape[3]
    mx = geo.gx * depth
    lx, ly = mx // 2, my // 2
    share = geo.bz // 4
    groups = LANES // share

    def kernel(in_ref, low_ref, out_values, out_coeff, out_weight, out_source, *scratch):
        coeff, values, scaled, diag, pairs = scratch
        rows = slice(PAD, PAD + my)
        for ref in (coeff, values, scaled):
            clear_mid(mx, my, ref)
        for block in range(geo.gx):
            span = slice(block * depth, (block + 1) * depth)
            scaled_block = 0.5 * in_ref[block, 1]
            coeff[1 + block * depth : 1 + (block + 1) * depth, rows, :] = scaled_block
            out_coeff[span] = scaled_block
            out_source[span] = 4.0 * in_ref[block, 0]

        def first_red(row, cell, red):
            mine = coeff[row, rows, :]
            total = 6.0 * mine + mid_sum(my, coeff, row)
            inverse = jnp.where(mine > 0.0, 1.0 / total, 0.0)
            diag[cell] = total
            out_weight[cell] = inverse
            fresh = jnp.where(red, inverse * out_source[cell], 0.0)
            values[row, rows, :] = fresh
            scaled[row, rows, :] = mine * fresh

        mid_rows(mx, my, first_red)
        for colour in (1, 0, 1):
            mid_half(mx, my, colour, coeff, out_weight, out_source, values, scaled)

        def residual(row, cell, red):
            mine = coeff[row, rows, :]
            here = values[row, rows, :]
            summed = mine * mid_sum(my, values, row) + mid_sum(my, scaled, row)
            left = 0.25 * (out_source[cell] + summed - diag[cell] * here)
            pairs[cell] = jnp.where(red, left, 0.0)
            out_values[cell] = here

        mid_rows(mx, my, residual)

        source_lane = iota((LANES, LANES), 0)
        target_lane = iota((LANES, LANES), 1)
        for which in (0, 1):
            for cell in range(lx):
                if which == 0:
                    pair = pairs[2 * cell] + pairs[2 * cell + 1]
                else:
                    pair = out_coeff[2 * cell] + out_coeff[2 * cell + 1]
                diag[cell] = pair
            total = jnp.zeros((lx // groups * ly, LANES), F32)
            for group in range(groups):
                parts = []
                for cell in range(group, lx, groups):
                    low = diag[cell, pl.ds(0, ly, 2), :]
                    high = diag[cell, pl.ds(1, ly, 2), :]
                    parts.append(low + high)
                stacked = jnp.concatenate(parts, axis=0)
                fold = (target_lane == source_lane // 2 + group * share) & (
                    source_lane < 2 * share
                )
                total = total + exact_dot(stacked, jnp.where(fold, 0.125, 0.0))
            low_ref[which] = total.reshape(lx // groups, ly, LANES)

    full = shape_f32(mx, my, LANES)
    padded = pltpu.VMEM((mx + 2, my + 2 * PAD, LANES), F32)
    plain = pltpu.VMEM((mx, my, LANES), F32)
    return call(
        kernel,
        [shape_f32(2, lx // groups, ly, LANES), full, full, full, full],
        [padded] * 3 + [plain] * 2,
    )(gathered)


def low_shift(values, dim, step):
    size = values.shape[dim]
    if dim == 0:
        blank = jnp.zeros_like(values[0:1])
        if step < 0:
            return jnp.concatenate([blank, values[:-1]], axis=0)
        return jnp.concatenate([values[1:], blank], axis=0)
    turned = pltpu.roll(values, 1 if step < 0 else size - 1, dim)
    edge = 0 if step < 0 else size - 1
    return jnp.where(iota(values.shape, dim) == edge, 0.0, turned)


def low_sum(values):
    total = low_shift(values, 0, -1) + low_shift(values, 0, 1)
    for dim in (1, 2):
        total = total + low_shift(values, dim, -1) + low_shift(values, dim, 1)
    return total


def bottom_solve(rhs, half_coeff):
    diag = 6.0 * half_coeff + low_sum(half_coeff)

    def apply(values):
        summed = half_coeff * low_sum(values) + low_sum(half_coeff * values)
        return (diag * values - summed) * 0.0625

    image = apply(rhs)
    alpha = jnp.sum(rhs * rhs) / jnp.sum(rhs * image)
    rest = rhs - alpha * image
    turned = apply(rest)
    omega = jnp.sum(turned * rest) / jnp.sum(turned * turned)
    return alpha * rhs + omega * rest


def finish(geo, lows, mids, fines):
    mx, my = mids[0].shape[0], mids[0].shape[1]
    lx, ly = mx // 2, my // 2
    share = geo.bz // 4
    groups = LANES // share
    columns = geo.gz * share
    wx, wy = geo.wx, geo.wy
    cx, cy = geo.bx // 2, geo.by // 2
    reach = HALO // 2

    def kernel(*refs):
        low_ref = refs[0]
        mid_values, mid_coeff, mid_weight, mid_source = refs[1:5]
        fine_black, fine_coeff, fine_weight, fine_source = refs[5:9]
        out_ref = refs[9]
        low_full, spread, mc, mv, mw, up = refs[10:16]
        kr, kb, vr, vb, wr, wb = refs[16:]

        lane = iota((ly, LANES), 1) // share
        for which in (0, 1):
            for cell in range(lx):
                line, group = cell // groups, cell % groups
                for tile in range(columns // LANES):
                    total = jnp.zeros((ly, LANES), F32)
                    for part in range(groups):
                        piece = low_ref[tile * groups + part, which, line]
                        shift = ((part - group) * share) % LANES
                        if shift:
                            piece = pltpu.roll(piece, shift, 1)
                        total = jnp.where(lane == part, piece, total)
                    low_full[which, cell, :, tile * LANES : (tile + 1) * LANES] = total
        bottom = bottom_solve(low_full[0], low_full[1])

        target = iota((columns, LANES), 1)
        target = jnp.where(target < LANES // 2 + LANES // 4, target, target - LANES)
        wanted = (target + LANES) // 2 - LANES // 2 + lax.axis_index("gz") * share
        copy = (iota((columns, LANES), 0) == wanted).astype(F32)
        fetched = exact_dot(bottom.reshape(lx * ly, columns), copy).reshape(lx, ly, LANES)
        rows = slice(PAD, PAD + my)
        for ref in (mc, mv, mw):
            clear_mid(mx, my, ref)
        for cell in range(lx):
            spread[cell, pl.ds(0, ly, 2), :] = fetched[cell]
            spread[cell, pl.ds(1, ly, 2), :] = fetched[cell]
        for cell in range(mx):
            mine = mid_coeff[cell]
            fresh = mid_values[cell] + spread[cell // 2]
            mc[cell + 1, rows, :] = mine
            mv[cell + 1, rows, :] = fresh
            mw[cell + 1, rows, :] = mine * fresh
        for colour in (0, 1, 0, 1):
            mid_half(mx, my, colour, mc, mid_weight, mid_source, mv, mw)

        up[...] = jnp.zeros_like(up)
        first = lax.axis_index("gx") * cx - reach
        for cell in range(wx // 2):
            at = first + cell
            clipped = jnp.clip(at, 0, mx - 1)
            line = mv[clipped + 1, rows, :]
            line = jnp.where((at >= 0) & (at < mx), line, 0.0)
            up[cell, pl.ds(PAD, my, 2), :] = line
            up[cell, pl.ds(PAD + 1, my, 2), :] = line
        for ref in (kr, kb, vr, vb, wr, wb):
            clear_pads(geo, ref)
        begin = PAD + lax.axis_index("gy") * geo.by - geo.own_y()
        begin = pl.multiple_of(begin, HALO)
        inner = slice(PAD, PAD + wy)
        for cell in range(wx):
            red, black = fine_coeff[0, cell], fine_coeff[1, cell]
            kr[cell + 1, inner, :] = red
            kb[cell + 1, inner, :] = black
            lifted = jnp.where(black > 0.0, up[cell // 2, pl.ds(begin, wy), :], 0.0)
            fresh = fine_black[cell] + lifted
            vb[cell + 1, inner, :] = fresh
            wb[cell + 1, inner, :] = black * fresh
        coeff, values, scaled = (kr, kb), (vr, vb), (wr, wb)
        weight = (fine_weight.at[0], fine_weight.at[1])
        source = (fine_source.at[0], fine_source.at[1])
        for colour in (0, 1, 0, 1):
            fine_half(geo, colour, coeff, weight, source, values, scaled)

        own = pl.multiple_of(geo.own_y() + PAD, HALO)
        span = slice(HALO + 1, HALO + 1 + geo.bx)
        red = vr[span, pl.ds(own, geo.by), :]
        black = vb[span, pl.ds(own, geo.by), :]
        even_first = even_rows((geo.bx, geo.by, LANES), (0, 1))
        even = jnp.where(even_first, red, black).reshape(geo.bx * geo.by, LANES)
        odd = jnp.where(even_first, black, red).reshape(geo.bx * geo.by, LANES)
        from_lane = iota((LANES, geo.bz), 0)
        to_lane = iota((LANES, geo.bz), 1)
        result = exact_dot(even, (to_lane == 2 * from_lane).astype(F32))
        result = result + exact_dot(odd, (to_lane == 2 * from_lane + 1).astype(F32))
        out_ref[...] = result.reshape(geo.bx, geo.by, geo.bz)

    padded = pltpu.VMEM((mx + 2, my + 2 * PAD, LANES), F32)
    return call(
        kernel,
        shape_f32(geo.bx, geo.by, geo.bz),
        [
            pltpu.VMEM((2, lx, ly, columns), F32),
            pltpu.VMEM((lx, my, LANES), F32),
            padded,
            padded,
            padded,
            pltpu.VMEM((wx // 2, 2 * my + 2 * PAD, LANES), F32),
        ]
        + [fine_scratch(geo)] * 6,
    )(lows, *mids, *fines)


def gather_coarse(geo, coarse):
    if geo.swap:
        other = lax.ppermute(coarse, "gy", [(0, 1), (1, 0)])
        lower = lax.axis_index("gy") == 0
        rows = jnp.concatenate(
            [jnp.where(lower, coarse, other), jnp.where(lower, other, coarse)], axis=2
        )
    else:
        rows = lax.all_gather(coarse, "gy", axis=2, tiled=True)
    return lax.all_gather(rows, "gx", axis=0, tiled=False)


def per_device(geo, old_slots, old_ids, coefficient):
    before = lax.ppermute(coefficient, "gz", neighbours_of("gz", geo.gz, 1))
    after = lax.ppermute(coefficient, "gz", neighbours_of("gz", geo.gz, -1))
    capacity, cells = old_slots.shape[2], old_slots.shape[3]
    tags = jnp.broadcast_to(old_ids.reshape(capacity, 1), (capacity, LANES)).astype(BF16)
    tagged = jnp.concatenate([old_slots.reshape(capacity, cells), tags], axis=1)
    column = lax.all_gather(tagged, "gz", axis=0, tiled=True)

    own_k, *send_k = pack_coefficient(geo, coefficient, before, after)
    halo_k = exchange_y(geo, send_k)
    own_f, *send_f = pack_source(geo, column, cells)
    halo_f = exchange_y(geo, send_f)
    low_k, high_k = widen_y(geo, own_k, halo_k)
    left_k, right_k = exchange_x(geo, low_k, high_k)
    low_f, high_f = widen_y(geo, own_f, halo_f)
    left_f, right_f = exchange_x(geo, low_f, high_f)

    coarse, *fines = fine_before(
        geo, (left_k, low_k, high_k, right_k), (left_f, low_f, high_f, right_f)
    )
    packed, *mids = mid_before(geo, gather_coarse(geo, coarse))
    lows = lax.all_gather(packed, "gz", axis=0, tiled=False)
    return finish(geo, lows, mids, fines)


def solution(mesh):
    sizes = tuple(mesh.shape[name] for name in ("gx", "gy", "gz"))

    def body(old_slots, old_ids, old_owner, coefficient):
        del old_owner
        geo = Geometry(sizes, coefficient.shape)
        return per_device(geo, old_slots, old_ids, coefficient)

    in_specs = (
        P("gx", "gy", "gz", None),
        P("gx", "gy", "gz"),
        P("gx", "gy", None),
        P("gx", "gy", "gz"),
    )
    return jax.shard_map(
        body, mesh=mesh, in_specs=in_specs, out_specs=P("gx", "gy", "gz"), check_vma=False
    )
```

```python
import jax
import jax.numpy as jnp
from jax import lax
from jax.experimental import pallas as pl
from jax.experimental.pallas import tpu as pltpu
from jax.sharding import PartitionSpec as P

BOX = 16
HALO = 8
LANES = 128
UNROLL = 16
HIGH = lax.Precision.HIGHEST
F32 = jnp.float32
BF16 = jnp.bfloat16


def iota(shape, dim):
    return lax.broadcasted_iota(jnp.int32, shape, dim)


def exact_dot(left, right):
    return lax.dot_general(
        left, right, (((1,), (0,)), ((), ())), precision=HIGH, preferred_element_type=F32
    )


def even_rows(shape, dims):
    total = iota(shape, dims[0])
    for dim in dims[1:]:
        total = total + iota(shape, dim)
    return total % 2 == 0


def call(kernel, outs, scratch=(), **more):
    return pl.pallas_call(
        kernel,
        out_shape=outs,
        scratch_shapes=list(scratch),
        compiler_params=pltpu.CompilerParams(vmem_limit_bytes=48 * 1024 * 1024),
        **more,
    )


def shape_f32(*dims):
    return jax.ShapeDtypeStruct(dims, F32)


class Geometry:
    def __init__(self, sizes, block):
        self.gx, self.gy, self.gz = sizes
        self.bx, self.by, self.bz = block
        self.swap = self.gy == 2
        self.wx = self.bx + 2 * HALO
        self.wy = self.by + (HALO if self.swap else 2 * HALO)

    def own_y(self):
        if self.swap:
            return pl.multiple_of(lax.axis_index("gy") * HALO, HALO)
        return HALO

    def halo_y(self):
        if self.swap:
            return (pl.multiple_of((1 - lax.axis_index("gy")) * self.by, HALO),)
        return (0, HALO + self.by)


def neighbours_of(axis, count, step):
    if step > 0:
        return [(i, i + 1) for i in range(count - 1)]
    return [(i + 1, i) for i in range(count - 1)]


def pack_coefficient(geo, own, before, after):
    bx, by, bz = geo.bx, geo.by, geo.bz
    half = bz // 2

    def kernel(own_ref, before_ref, after_ref, out_ref, *sends):
        rows = bx * by
        lane = iota((rows, bz), 1)
        mine = own_ref[...].reshape(rows, bz)
        near = jnp.where(
            lane < half, after_ref[...].reshape(rows, bz), before_ref[...].reshape(rows, bz)
        )
        source = iota((bz, LANES), 0)
        target = iota((bz, LANES), 1)

        def pick(shift):
            low = (source == 2 * target + shift).astype(F32)
            high = (source == 2 * target + shift - bz).astype(F32)
            return exact_dot(mine, low) + exact_dot(near, high)

        even = pick(0).reshape(bx, by, LANES)
        odd = pick(1).reshape(bx, by, LANES)
        first = even_rows((bx, by, LANES), (0, 1))
        out_ref[0] = jnp.where(first, even, odd)
        out_ref[1] = jnp.where(first, odd, even)
        emit_sends(geo, out_ref, sends)

    return call(kernel, [shape_f32(2, bx, by, LANES)] + send_shapes(geo))(own, before, after)


def send_shapes(geo):
    one = shape_f32(2, geo.bx, HALO, LANES)
    return [one] if geo.swap else [one, one]


def emit_sends(geo, out_ref, sends):
    top = geo.by - HALO
    if geo.swap:
        start = pl.multiple_of((1 - lax.axis_index("gy")) * top, HALO)
        sends[0][...] = out_ref[:, :, pl.ds(start, HALO), :]
    else:
        sends[0][...] = out_ref[:, :, 0:HALO, :]
        sends[1][...] = out_ref[:, :, top : top + HALO, :]


def pack_source(geo, slots, cells):
    bx, by = geo.bx, geo.by
    count = slots.shape[0]
    tiles = cells // LANES
    boxes = 2 * geo.bz // BOX
    own_boxes = geo.bz // BOX
    per_tile = LANES // BOX
    pair = BOX // 2

    def kernel(slot_ref, out_ref, *rest):
        sends, ordered = rest[:-1], rest[-1]
        ids = slot_ref[:, cells : cells + LANES].astype(F32)
        place = iota((count, LANES), 1)
        wanted = jnp.where(place < own_boxes + own_boxes // 2, place, place - boxes)
        wanted = (wanted + lax.axis_index("gz") * own_boxes).astype(F32)
        chosen = jnp.where((ids == wanted) & (ids >= 0.0) & (place < boxes), 1.0, 0.0)
        chosen = chosen.T[0:boxes].astype(BF16)
        for tile in range(tiles):
            ordered[tile] = jnp.dot(
                chosen,
                slot_ref[:, tile * LANES : (tile + 1) * LANES],
                preferred_element_type=F32,
            )
        rows = tiles * per_tile
        keep = iota((tiles, per_tile, LANES), 2) // BOX == iota((tiles, per_tile, LANES), 1)
        inside = iota((LANES, 2 * LANES), 0) % BOX
        target = iota((LANES, 2 * LANES), 1)
        slot_of = jnp.where(
            inside % 2 == 0, inside // 2, inside // 2 + LANES
        )
        total = jnp.zeros((rows, 2 * LANES), F32)
        for box in range(boxes):
            line = jnp.broadcast_to(ordered[:, box : box + 1, :], (tiles, per_tile, LANES))
            line = jnp.where(keep, line, 0.0).reshape(rows, LANES).astype(BF16)
            spread = (target == slot_of + box * pair).astype(F32).astype(BF16)
            total = total + jnp.dot(line, spread, preferred_element_type=F32)
        even = total[:, 0:LANES].reshape(bx, by, LANES)
        odd = total[:, LANES:].reshape(bx, by, LANES)
        first = even_rows((bx, by, LANES), (0, 1))
        out_ref[0] = jnp.where(first, even, odd)
        out_ref[1] = jnp.where(first, odd, even)
        emit_sends(geo, out_ref, sends)

    return call(
        kernel,
        [shape_f32(2, bx, by, LANES)] + send_shapes(geo),
        [pltpu.VMEM((tiles, boxes, LANES), F32)],
    )(slots)


def exchange_y(geo, sends):
    if geo.swap:
        return (lax.ppermute(sends[0], "gy", [(0, 1), (1, 0)]),)
    low, high = sends
    return (
        lax.ppermute(high, "gy", neighbours_of("gy", geo.gy, 1)),
        lax.ppermute(low, "gy", neighbours_of("gy", geo.gy, -1)),
    )


def widen_y(geo, own, halos):
    half = geo.bx // 2

    def kernel(own_ref, *rest):
        halo_refs, outs = rest[:-2], rest[-2:]
        for part, out in enumerate(outs):
            span = slice(part * half, (part + 1) * half)
            out[:, :, pl.ds(geo.own_y(), geo.by), :] = own_ref[:, span]
            for halo, start in zip(halo_refs, geo.halo_y()):
                out[:, :, pl.ds(start, HALO), :] = halo[:, span]

    slab = shape_f32(2, half, geo.wy, LANES)
    return call(kernel, [slab, slab])(own, *halos)


def exchange_x(geo, low, high):
    return (
        lax.ppermute(high, "gx", neighbours_of("gx", geo.gx, 1)),
        lax.ppermute(low, "gx", neighbours_of("gx", geo.gx, -1)),
    )


PAD = 8


def fine_sum(geo, ref, row, near_low):
    rows = slice(PAD, PAD + geo.wy)
    here = ref[row, rows, :]
    total = ref[row - 1, rows, :] + ref[row + 1, rows, :] + here
    total = total + ref[row, PAD - 1 : PAD - 1 + geo.wy, :]
    total = total + ref[row, PAD + 1 : PAD + 1 + geo.wy, :]
    low = pltpu.roll(here, 1, 1)
    high = pltpu.roll(here, LANES - 1, 1)
    return total + jnp.where(near_low, low, high)


def fine_rows(geo, body):
    even = iota((geo.wy, LANES), 0) % 2 == 0
    odd = jnp.logical_not(even)

    def step(index, carry):
        body(2 * index + 1, 2 * index, even)
        body(2 * index + 2, 2 * index + 1, odd)
        return carry

    lax.fori_loop(0, geo.wx // 2, step, 0, unroll=UNROLL)


def fine_half(geo, colour, coeff, weight, source, values, scaled, extra=None):
    other = 1 - colour

    def body(row, cell, low):
        near_low = low if colour == 0 else jnp.logical_not(low)
        rows = slice(PAD, PAD + geo.wy)
        mine = coeff[colour][row, rows, :]
        summed = mine * fine_sum(geo, values[other], row, near_low)
        summed = summed + fine_sum(geo, scaled[other], row, near_low)
        fresh = weight[colour][cell] * (source[colour][cell] + summed)
        values[colour][row, rows, :] = fresh
        scaled[colour][row, rows, :] = mine * fresh

    fine_rows(geo, body)


def clear_pads(geo, ref):
    blank_row = jnp.zeros((geo.wy + 2 * PAD, LANES), F32)
    ref[0] = blank_row
    ref[geo.wx + 1] = blank_row
    edge = jnp.zeros((geo.wx + 2, PAD, LANES), F32)
    ref[:, 0:PAD, :] = edge
    ref[:, PAD + geo.wy : PAD + geo.wy + PAD, :] = edge


def fine_scratch(geo):
    return pltpu.VMEM((geo.wx + 2, geo.wy + 2 * PAD, LANES), F32)


def fine_before(geo, coefficient, source):
    half = geo.bx // 2
    wx, wy = geo.wx, geo.wy
    cx, cy = geo.bx // 2, geo.by // 2

    def kernel(*refs):
        coeff_in, source_in = refs[0:4], refs[4:8]
        coarse_ref, out_black, out_coeff, out_weight, out_source = refs[8:13]
        kr, kb, vr, vb, wr, wb, diag, resid = refs[13:]
        coeff, values, scaled = (kr, kb), (vr, vb), (wr, wb)
        rows = slice(PAD, PAD + wy)
        for ref in (kr, kb, vr, vb, wr, wb):
            clear_pads(geo, ref)
        start = 0
        for slab, slab_source in zip(coeff_in, source_in):
            depth = slab.shape[1]
            for colour in (0, 1):
                scaled_slab = 0.5 * slab[colour]
                coeff[colour][1 + start : 1 + start + depth, rows, :] = scaled_slab
                out_coeff[colour, start : start + depth] = scaled_slab
                out_source[colour, start : start + depth] = slab_source[colour]
            start += depth
        weight = (out_weight.at[0], out_weight.at[1])
        source_at = (out_source.at[0], out_source.at[1])

        def first_red(row, cell, low):
            mine = kr[row, rows, :]
            total = 6.0 * mine + fine_sum(geo, kb, row, low)
            inverse = jnp.where(mine > 0.0, 1.0 / total, 0.0)
            diag[cell] = total
            out_weight[0, cell] = inverse
            fresh = inverse * out_source[0, cell]
            vr[row, rows, :] = fresh
            wr[row, rows, :] = mine * fresh

        fine_rows(geo, first_red)

        def first_black(row, cell, low):
            high = jnp.logical_not(low)
            mine = kb[row, rows, :]
            total = 6.0 * mine + fine_sum(geo, kr, row, high)
            inverse = jnp.where(mine > 0.0, 1.0 / total, 0.0)
            out_weight[1, cell] = inverse

        fine_rows(geo, first_black)
        fine_half(geo, 1, coeff, weight, source_at, values, scaled)
        fine_half(geo, 0, coeff, weight, source_at, values, scaled)
        fine_half(geo, 1, coeff, weight, source_at, values, scaled)

        def residual(row, cell, low):
            mine = kr[row, rows, :]
            summed = mine * fine_sum(geo, vb, row, low) + fine_sum(geo, wb, row, low)
            resid[cell] = out_source[0, cell] + summed - diag[cell] * vr[row, rows, :]
            out_black[cell] = vb[row, rows, :]

        fine_rows(geo, residual)

        own = geo.own_y()
        for cell in range(cx):
            at = HALO + 2 * cell
            pair = resid[at] + resid[at + 1]
            diag[at] = pair
            mine = kr[at + 1, rows, :] + kr[at + 2, rows, :]
            mine = mine + kb[at + 1, rows, :] + kb[at + 2, rows, :]
            diag[at + 1] = mine
            for which, scale in ((0, 0.125), (1, 0.25)):
                low = diag[at + which, pl.ds(own, cy, 2), :]
                high = diag[at + which, pl.ds(own + 1, cy, 2), :]
                coarse_ref[which, cell] = scale * (low + high)

    window = shape_f32(wx, wy, LANES)
    both = shape_f32(2, wx, wy, LANES)
    return call(
        kernel,
        [shape_f32(2, cx, cy, LANES), window, both, both, both],
        [fine_scratch(geo)] * 6 + [pltpu.VMEM((wx, wy, LANES), F32)] * 2,
    )(*coefficient, *source)


def mid_sum(my, ref, row):
    rows = slice(PAD, PAD + my)
    here = ref[row, rows, :]
    total = ref[row - 1, rows, :] + ref[row + 1, rows, :]
    total = total + ref[row, PAD - 1 : PAD - 1 + my, :]
    total = total + ref[row, PAD + 1 : PAD + 1 + my, :]
    return total + pltpu.roll(here, 1, 1) + pltpu.roll(here, LANES - 1, 1)


def mid_rows(mx, my, body):
    even = (iota((my, LANES), 0) + iota((my, LANES), 1)) % 2 == 0
    odd = jnp.logical_not(even)

    def step(index, carry):
        body(2 * index + 1, 2 * index, even)
        body(2 * index + 2, 2 * index + 1, odd)
        return carry

    lax.fori_loop(0, mx // 2, step, 0, unroll=UNROLL)


def mid_half(mx, my, colour, coeff, weight, source, values, scaled):
    rows = slice(PAD, PAD + my)

    def body(row, cell, red):
        chosen = red if colour == 0 else jnp.logical_not(red)
        mine = coeff[row, rows, :]
        summed = mine * mid_sum(my, values, row) + mid_sum(my, scaled, row)
        fresh = weight[cell] * (source[cell] + summed)
        fresh = jnp.where(chosen, fresh, values[row, rows, :])
        values[row, rows, :] = fresh
        scaled[row, rows, :] = mine * fresh

    mid_rows(mx, my, body)


def clear_mid(mx, my, ref):
    ref[0] = jnp.zeros((my + 2 * PAD, LANES), F32)
    ref[mx + 1] = jnp.zeros((my + 2 * PAD, LANES), F32)
    edge = jnp.zeros((mx + 2, PAD, LANES), F32)
    ref[:, 0:PAD, :] = edge
    ref[:, PAD + my : PAD + my + PAD, :] = edge


def mid_before(geo, gathered):
    depth, my = gathered.shape[2], gathered.shape[3]
    mx = geo.gx * depth
    lx, ly = mx // 2, my // 2
    share = geo.bz // 4
    groups = LANES // share

    def kernel(in_ref, low_ref, out_values, out_coeff, out_weight, out_source, *scratch):
        coeff, values, scaled, diag, pairs = scratch
        rows = slice(PAD, PAD + my)
        for ref in (coeff, values, scaled):
            clear_mid(mx, my, ref)
        for block in range(geo.gx):
            span = slice(block * depth, (block + 1) * depth)
            scaled_block = 0.5 * in_ref[block, 1]
            coeff[1 + block * depth : 1 + (block + 1) * depth, rows, :] = scaled_block
            out_coeff[span] = scaled_block
            out_source[span] = 4.0 * in_ref[block, 0]

        def first_red(row, cell, red):
            mine = coeff[row, rows, :]
            total = 6.0 * mine + mid_sum(my, coeff, row)
            inverse = jnp.where(mine > 0.0, 1.0 / total, 0.0)
            diag[cell] = total
            out_weight[cell] = inverse
            fresh = jnp.where(red, inverse * out_source[cell], 0.0)
            values[row, rows, :] = fresh
            scaled[row, rows, :] = mine * fresh

        mid_rows(mx, my, first_red)
        for colour in (1, 0, 1):
            mid_half(mx, my, colour, coeff, out_weight, out_source, values, scaled)

        def residual(row, cell, red):
            mine = coeff[row, rows, :]
            here = values[row, rows, :]
            summed = mine * mid_sum(my, values, row) + mid_sum(my, scaled, row)
            left = 0.25 * (out_source[cell] + summed - diag[cell] * here)
            pairs[cell] = jnp.where(red, left, 0.0)
            out_values[cell] = here

        mid_rows(mx, my, residual)

        source_lane = iota((LANES, LANES), 0)
        target_lane = iota((LANES, LANES), 1)
        for which in (0, 1):
            for cell in range(lx):
                if which == 0:
                    pair = pairs[2 * cell] + pairs[2 * cell + 1]
                else:
                    pair = out_coeff[2 * cell] + out_coeff[2 * cell + 1]
                diag[cell] = pair
            total = jnp.zeros((lx // groups * ly, LANES), F32)
            for group in range(groups):
                parts = []
                for cell in range(group, lx, groups):
                    low = diag[cell, pl.ds(0, ly, 2), :]
                    high = diag[cell, pl.ds(1, ly, 2), :]
                    parts.append(low + high)
                stacked = jnp.concatenate(parts, axis=0)
                fold = (target_lane == source_lane // 2 + group * share) & (
                    source_lane < 2 * share
                )
                total = total + exact_dot(stacked, jnp.where(fold, 0.125, 0.0))
            low_ref[which] = total.reshape(lx // groups, ly, LANES)

    full = shape_f32(mx, my, LANES)
    padded = pltpu.VMEM((mx + 2, my + 2 * PAD, LANES), F32)
    plain = pltpu.VMEM((mx, my, LANES), F32)
    return call(
        kernel,
        [shape_f32(2, lx // groups, ly, LANES), full, full, full, full],
        [padded] * 3 + [plain] * 2,
    )(gathered)


def low_shift(values, dim, step):
    size = values.shape[dim]
    if dim == 0:
        blank = jnp.zeros_like(values[0:1])
        if step < 0:
            return jnp.concatenate([blank, values[:-1]], axis=0)
        return jnp.concatenate([values[1:], blank], axis=0)
    turned = pltpu.roll(values, 1 if step < 0 else size - 1, dim)
    edge = 0 if step < 0 else size - 1
    return jnp.where(iota(values.shape, dim) == edge, 0.0, turned)


def low_sum(values):
    total = low_shift(values, 0, -1) + low_shift(values, 0, 1)
    for dim in (1, 2):
        total = total + low_shift(values, dim, -1) + low_shift(values, dim, 1)
    return total


def bottom_solve(rhs, half_coeff):
    diag = 6.0 * half_coeff + low_sum(half_coeff)

    def apply(values):
        summed = half_coeff * low_sum(values) + low_sum(half_coeff * values)
        return (diag * values - summed) * 0.0625

    image = apply(rhs)
    alpha = jnp.sum(rhs * rhs) / jnp.sum(rhs * image)
    rest = rhs - alpha * image
    turned = apply(rest)
    omega = jnp.sum(turned * rest) / jnp.sum(turned * turned)
    return alpha * rhs + omega * rest


def finish(geo, lows, mids, fines):
    mx, my = mids[0].shape[0], mids[0].shape[1]
    lx, ly = mx // 2, my // 2
    share = geo.bz // 4
    groups = LANES // share
    columns = geo.gz * share
    wx, wy = geo.wx, geo.wy
    cx, cy = geo.bx // 2, geo.by // 2
    reach = HALO // 2

    def kernel(*refs):
        low_ref = refs[0]
        mid_values, mid_coeff, mid_weight, mid_source = refs[1:5]
        fine_black, fine_coeff, fine_weight, fine_source = refs[5:9]
        out_ref = refs[9]
        low_full, spread, mc, mv, mw, up = refs[10:16]
        kr, kb, vr, vb, wr, wb = refs[16:]

        lane = iota((ly, LANES), 1) // share
        for which in (0, 1):
            for cell in range(lx):
                line, group = cell // groups, cell % groups
                for tile in range(columns // LANES):
                    total = jnp.zeros((ly, LANES), F32)
                    for part in range(groups):
                        piece = low_ref[tile * groups + part, which, line]
                        shift = ((part - group) * share) % LANES
                        if shift:
                            piece = pltpu.roll(piece, shift, 1)
                        total = jnp.where(lane == part, piece, total)
                    low_full[which, cell, :, tile * LANES : (tile + 1) * LANES] = total
        bottom = bottom_solve(low_full[0], low_full[1])

        target = iota((columns, LANES), 1)
        target = jnp.where(target < LANES // 2 + LANES // 4, target, target - LANES)
        wanted = (target + LANES) // 2 - LANES // 2 + lax.axis_index("gz") * share
        copy = (iota((columns, LANES), 0) == wanted).astype(F32)
        fetched = exact_dot(bottom.reshape(lx * ly, columns), copy).reshape(lx, ly, LANES)
        rows = slice(PAD, PAD + my)
        for ref in (mc, mv, mw):
            clear_mid(mx, my, ref)
        for cell in range(lx):
            spread[cell, pl.ds(0, ly, 2), :] = fetched[cell]
            spread[cell, pl.ds(1, ly, 2), :] = fetched[cell]
        for cell in range(mx):
            mine = mid_coeff[cell]
            fresh = mid_values[cell] + spread[cell // 2]
            mc[cell + 1, rows, :] = mine
            mv[cell + 1, rows, :] = fresh
            mw[cell + 1, rows, :] = mine * fresh
        for colour in (0, 1, 0, 1):
            mid_half(mx, my, colour, mc, mid_weight, mid_source, mv, mw)

        up[...] = jnp.zeros_like(up)
        first = lax.axis_index("gx") * cx - reach
        for cell in range(wx // 2):
            at = first + cell
            clipped = jnp.clip(at, 0, mx - 1)
            line = mv[clipped + 1, rows, :]
            line = jnp.where((at >= 0) & (at < mx), line, 0.0)
            up[cell, pl.ds(PAD, my, 2), :] = line
            up[cell, pl.ds(PAD + 1, my, 2), :] = line
        for ref in (kr, kb, vr, vb, wr, wb):
            clear_pads(geo, ref)
        begin = PAD + lax.axis_index("gy") * geo.by - geo.own_y()
        begin = pl.multiple_of(begin, HALO)
        inner = slice(PAD, PAD + wy)
        for cell in range(wx):
            red, black = fine_coeff[0, cell], fine_coeff[1, cell]
            kr[cell + 1, inner, :] = red
            kb[cell + 1, inner, :] = black
            lifted = jnp.where(black > 0.0, up[cell // 2, pl.ds(begin, wy), :], 0.0)
            fresh = fine_black[cell] + lifted
            vb[cell + 1, inner, :] = fresh
            wb[cell + 1, inner, :] = black * fresh
        coeff, values, scaled = (kr, kb), (vr, vb), (wr, wb)
        weight = (fine_weight.at[0], fine_weight.at[1])
        source = (fine_source.at[0], fine_source.at[1])
        for colour in (0, 1, 0, 1):
            fine_half(geo, colour, coeff, weight, source, values, scaled)

        own = pl.multiple_of(geo.own_y() + PAD, HALO)
        span = slice(HALO + 1, HALO + 1 + geo.bx)
        red = vr[span, pl.ds(own, geo.by), :]
        black = vb[span, pl.ds(own, geo.by), :]
        even_first = even_rows((geo.bx, geo.by, LANES), (0, 1))
        even = jnp.where(even_first, red, black).reshape(geo.bx * geo.by, LANES)
        odd = jnp.where(even_first, black, red).reshape(geo.bx * geo.by, LANES)
        from_lane = iota((LANES, geo.bz), 0)
        to_lane = iota((LANES, geo.bz), 1)
        result = exact_dot(even, (to_lane == 2 * from_lane).astype(F32))
        result = result + exact_dot(odd, (to_lane == 2 * from_lane + 1).astype(F32))
        out_ref[...] = result.reshape(geo.bx, geo.by, geo.bz)

    padded = pltpu.VMEM((mx + 2, my + 2 * PAD, LANES), F32)
    return call(
        kernel,
        shape_f32(geo.bx, geo.by, geo.bz),
        [
            pltpu.VMEM((2, lx, ly, columns), F32),
            pltpu.VMEM((lx, my, LANES), F32),
            padded,
            padded,
            padded,
            pltpu.VMEM((wx // 2, 2 * my + 2 * PAD, LANES), F32),
        ]
        + [fine_scratch(geo)] * 6,
    )(lows, *mids, *fines)


def gather_coarse(geo, coarse):
    if geo.swap:
        other = lax.ppermute(coarse, "gy", [(0, 1), (1, 0)])
        lower = lax.axis_index("gy") == 0
        rows = jnp.concatenate(
            [jnp.where(lower, coarse, other), jnp.where(lower, other, coarse)], axis=2
        )
    else:
        rows = lax.all_gather(coarse, "gy", axis=2, tiled=True)
    return lax.all_gather(rows, "gx", axis=0, tiled=False)


def per_device(geo, old_slots, old_ids, coefficient):
    before = lax.ppermute(coefficient, "gz", neighbours_of("gz", geo.gz, 1))
    after = lax.ppermute(coefficient, "gz", neighbours_of("gz", geo.gz, -1))
    capacity, cells = old_slots.shape[2], old_slots.shape[3]
    tags = jnp.broadcast_to(old_ids.reshape(capacity, 1), (capacity, LANES)).astype(BF16)
    tagged = jnp.concatenate([old_slots.reshape(capacity, cells), tags], axis=1)
    column = lax.all_gather(tagged, "gz", axis=0, tiled=True)

    own_k, *send_k = pack_coefficient(geo, coefficient, before, after)
    halo_k = exchange_y(geo, send_k)
    own_f, *send_f = pack_source(geo, column, cells)
    halo_f = exchange_y(geo, send_f)
    low_k, high_k = widen_y(geo, own_k, halo_k)
    left_k, right_k = exchange_x(geo, low_k, high_k)
    low_f, high_f = widen_y(geo, own_f, halo_f)
    left_f, right_f = exchange_x(geo, low_f, high_f)

    coarse, *fines = fine_before(
        geo, (left_k, low_k, high_k, right_k), (left_f, low_f, high_f, right_f)
    )
    packed, *mids = mid_before(geo, gather_coarse(geo, coarse))
    lows = lax.all_gather(packed, "gz", axis=0, tiled=False)
    return finish(geo, lows, mids, fines)


def solution(mesh):
    sizes = tuple(mesh.shape[name] for name in ("gx", "gy", "gz"))

    def body(old_slots, old_ids, old_owner, coefficient):
        del old_owner
        geo = Geometry(sizes, coefficient.shape)
        return per_device(geo, old_slots, old_ids, coefficient)

    in_specs = (
        P("gx", "gy", "gz", None),
        P("gx", "gy", "gz"),
        P("gx", "gy", None),
        P("gx", "gy", "gz"),
    )
    return jax.shard_map(
        body, mesh=mesh, in_specs=in_specs, out_specs=P("gx", "gy", "gz"), check_vma=False
    )
```

```python
import jax
import jax.numpy as jnp
from jax import lax
from jax.experimental import pallas as pl
from jax.experimental.pallas import tpu as pltpu
from jax.sharding import PartitionSpec as P


BOX = 16
SOURCE_ROWS = 12
COEFF_ROWS = SOURCE_ROWS + 1
MID_ROWS = 6
FINE_ROWS = 4
Z_PAIRS = 16
LANES = 128
HIGH = lax.Precision.HIGHEST
F32 = jnp.float32
BF16 = jnp.bfloat16


def iota(shape, dim):
    return lax.broadcasted_iota(jnp.int32, shape, dim)


def exact_dot(left, right):
    return lax.dot_general(
        left, right, (((1,), (0,)), ((), ())), precision=HIGH, preferred_element_type=F32
    )


def even_rows(shape, dims):
    total = iota(shape, dims[0])
    for dim in dims[1:]:
        total = total + iota(shape, dim)
    return total % 2 == 0


def call(kernel, outs, scratch=(), room=8):
    return pl.pallas_call(
        kernel,
        out_shape=outs,
        scratch_shapes=list(scratch),
        compiler_params=pltpu.CompilerParams(vmem_limit_bytes=room * 1024 * 1024),
    )


def shape_f32(*dims):
    return jax.ShapeDtypeStruct(dims, F32)


class Geometry:
    def __init__(self, sizes, block):
        self.gx, self.gy, self.gz = sizes
        self.bx, self.by, self.bz = block
        self.swap = self.gy == 2
        self.wx = 3 * self.bx
        self.wy = (2 if self.swap else 3) * self.by
        self.cx, self.cy = self.bx // 2, self.by // 2
        self.mx, self.my = self.wx // 2, self.wy // 2
        self.devices = self.gx * self.gy * self.gz
        self.fy = self.by + (8 if self.swap else 16)

    def kept_y(self):
        if self.swap:
            start = pl.multiple_of(lax.axis_index("gy") * 8, 8)
            return start, start
        return self.by - 8, 8

    def own_y(self, rows):
        if self.swap:
            return pl.multiple_of(lax.axis_index("gy") * rows, 8)
        return rows


def neighbours_of(count, step):
    if step > 0:
        return [(i, i + 1) for i in range(count - 1)]
    return [(i + 1, i) for i in range(count - 1)]


def from_neighbours(axis, count, low, high):
    return (
        lax.ppermute(high, axis, neighbours_of(count, 1)),
        lax.ppermute(low, axis, neighbours_of(count, -1)),
    )


def pack_coefficient(geo, own):
    bx, by, bz = geo.bx, geo.by, geo.bz
    half = bz // 2

    def kernel(own_ref, out_ref):
        source = iota((bz, bz), 0)
        target = iota((bz, bz), 1)
        wanted = jnp.where(target < half, 2 * target, 2 * (target - half) + 1)
        split = exact_dot(own_ref[...].reshape(bx * by, bz), (source == wanted).astype(F32))
        turned = pltpu.roll(split, half, 1)
        first = even_rows((bx, by, bz), (0, 1))
        out_ref[...] = jnp.where(
            first, split.reshape(bx, by, bz), turned.reshape(bx, by, bz)
        )

    return call(kernel, shape_f32(bx, by, bz))(own)


def widen_coefficient(geo, own):
    if not geo.swap:
        low, high = from_neighbours("gy", geo.gy, own, own)
        center = jnp.concatenate([low, own, high], axis=1)
        return center, center[:COEFF_ROWS], center[geo.bx - COEFF_ROWS :]
    other = lax.ppermute(own, "gy", [(0, 1), (1, 0)])

    def kernel(own_ref, other_ref, center, low, high):
        mine = geo.own_y(geo.by)
        start = pl.multiple_of(geo.by - mine, 8)
        center[:, pl.ds(mine, geo.by), :] = own_ref[...]
        center[:, pl.ds(start, geo.by), :] = other_ref[...]
        low[...] = center[0:COEFF_ROWS]
        high[...] = center[geo.bx - COEFF_ROWS :]

    slab = shape_f32(COEFF_ROWS, geo.wy, geo.bz)
    return call(kernel, [shape_f32(geo.bx, geo.wy, geo.bz), slab, slab])(own, other)


def coefficient_rows(geo):
    rows = [(0, i) for i in range(COEFF_ROWS)]
    rows += [(1, i) for i in range(geo.bx)]
    return rows + [(2, i) for i in range(COEFF_ROWS)]


def pack_ends(geo, parts):
    rows = coefficient_rows(geo)
    lines = -(-len(rows) // 4)

    def kernel(left, center, right, last, first):
        refs = (left, center, right)
        group = iota((geo.wy, LANES), 1) % (LANES // 2) // Z_PAIRS
        for line in range(lines):
            ends = jnp.zeros((geo.wy, LANES), F32)
            starts = ends
            for place, (part, row) in enumerate(rows[4 * line : 4 * line + 4]):
                value = refs[part][row]
                shift = place * Z_PAIRS
                down = pltpu.roll(value, LANES - shift, 1) if shift else value
                up = pltpu.roll(value, shift, 1) if shift else value
                ends = jnp.where(group == 3 - place, down, ends)
                starts = jnp.where(group == place, up, starts)
            last[line] = ends
            first[line] = starts

    packed = shape_f32(lines, geo.wy, LANES)
    return call(kernel, [packed, packed])(*parts)


def pack_source(geo, slots, cells, columns):
    bx, by = geo.bx, geo.by
    count = slots.shape[0] // columns
    tiles = cells // LANES
    boxes = 2 * geo.bz // BOX
    own_boxes = geo.bz // BOX
    per_tile = LANES // BOX
    pair = BOX // 2

    def kernel(slot_ref, center, low, high, *ordered_refs):
        place = iota((count, LANES), 1)
        wanted = jnp.where(place < own_boxes + own_boxes // 2, place, place - boxes)
        wanted = (wanted + lax.axis_index("gz") * own_boxes).astype(F32)
        rows = tiles * per_tile
        keep = iota((tiles, per_tile, LANES), 2) // BOX == iota((tiles, per_tile, LANES), 1)
        inside = iota((LANES, 2 * LANES), 0) % BOX
        target = iota((LANES, 2 * LANES), 1)
        slot_of = jnp.where(inside % 2 == 0, inside // 2, inside // 2 + LANES)
        first = even_rows((bx, by, LANES), (0, 1))
        for column, ordered in enumerate(ordered_refs):
            here = slice(column * count, (column + 1) * count)
            ids = slot_ref[here, cells : cells + LANES].astype(F32)
            chosen = (ids == wanted) & (ids >= 0.0) & (place < boxes)
            chosen = jnp.where(chosen, 1.0, 0.0).T[0:boxes].astype(BF16)
            for tile in range(tiles):
                ordered[tile] = jnp.dot(
                    chosen,
                    slot_ref[here, tile * LANES : (tile + 1) * LANES],
                    preferred_element_type=F32,
                )
            total = jnp.zeros((rows, 2 * LANES), F32)
            for box in range(boxes):
                line = ordered[:, box : box + 1, :]
                line = jnp.broadcast_to(line, (tiles, per_tile, LANES))
                line = jnp.where(keep, line, 0.0).reshape(rows, LANES).astype(BF16)
                spread = (target == slot_of + box * pair).astype(F32).astype(BF16)
                total = total + jnp.dot(line, spread, preferred_element_type=F32)
            even = total[:, 0:LANES].reshape(bx, by, LANES)
            odd = total[:, LANES:].reshape(bx, by, LANES)
            span = slice(column * by, (column + 1) * by)
            center[0, :, span, :] = jnp.where(first, even, odd).astype(BF16)
            center[1, :, span, :] = jnp.where(first, odd, even).astype(BF16)
        low[...] = center[:, 0:SOURCE_ROWS]
        high[...] = center[:, bx - SOURCE_ROWS :]

    def shape(rows):
        return jax.ShapeDtypeStruct((2, rows, columns * by, LANES), BF16)

    return call(
        kernel,
        [shape(bx), shape(SOURCE_ROWS), shape(SOURCE_ROWS)],
        [pltpu.VMEM((tiles, boxes, LANES), F32)] * columns,
        room=12,
    )(slots)


def tag_slots(slots, ids):
    capacity, cells = slots.shape

    def kernel(slot_ref, id_ref, out_ref):
        out_ref[:, 0:cells] = slot_ref[...]
        tags = jnp.broadcast_to(id_ref[...], (capacity, LANES))
        out_ref[:, cells:] = tags.astype(F32).astype(BF16)

    shape = jax.ShapeDtypeStruct((capacity, cells + LANES), BF16)
    return call(kernel, shape)(slots, ids)


def gather_source(geo, old_slots, old_ids):
    capacity, cells = old_slots.shape[2], old_slots.shape[3]
    slots, ids = old_slots.reshape(capacity, cells), old_ids.reshape(capacity, 1)
    axes = ("gy", "gz") if geo.swap else ("gz",)
    column = lax.all_gather(tag_slots(slots, ids), axes, axis=0, tiled=True)
    if geo.swap:
        return pack_source(geo, column, cells, 2)
    own = pack_source(geo, column, cells, 1)[0]
    low, high = from_neighbours("gy", geo.gy, own, own)
    center = jnp.concatenate([low, own, high], axis=2)
    return center, center[:, :SOURCE_ROWS], center[:, geo.bx - SOURCE_ROWS :]


PAD = 8


def padded(rows, width):
    return pltpu.VMEM((rows + 2, width + 2 * PAD, LANES), F32)


def clear_pads(ref):
    rows, width = ref.shape[0] - 2, ref.shape[1] - 2 * PAD
    ref[0] = jnp.zeros((width + 2 * PAD, LANES), F32)
    ref[rows + 1] = jnp.zeros((width + 2 * PAD, LANES), F32)
    edge = jnp.zeros((rows + 2, PAD, LANES), F32)
    ref[:, 0:PAD, :] = edge
    ref[:, PAD + width :, :] = edge


def inner(ref, row):
    return ref[row + 1, PAD : ref.shape[1] - PAD, :]


def put(ref, row, value):
    ref[row + 1, PAD : ref.shape[1] - PAD, :] = value


def across(ref, row):
    width = ref.shape[1] - 2 * PAD
    total = inner(ref, row - 1) + inner(ref, row + 1)
    total = total + ref[row + 1, PAD - 1 : PAD - 1 + width, :]
    return total + ref[row + 1, PAD + 1 : PAD + 1 + width, :]


def fine_sum(ref, row, near_low):
    here = inner(ref, row)
    low = pltpu.roll(here, 1, 1)
    high = pltpu.roll(here, LANES - 1, 1)
    return across(ref, row) + here + jnp.where(near_low, low, high)


def mid_sum(ref, row):
    here = inner(ref, row)
    return across(ref, row) + pltpu.roll(here, 1, 1) + pltpu.roll(here, LANES - 1, 1)


def over_rows(span, mask, body):
    first, last = span
    flipped = jnp.logical_not(mask)

    def step(index, carry):
        body(first + 2 * index, mask)
        body(first + 2 * index + 1, flipped)
        return carry

    lax.fori_loop(0, (last - first) // 2, step, 0, unroll=(last - first) // 2)


def low_rows(width):
    return iota((width, LANES), 0) % 2 == 0


def red_lanes(width):
    return (iota((width, LANES), 0) + iota((width, LANES), 1)) % 2 == 0


def weights(coeff_row, total):
    return jnp.where(coeff_row > 0.0, 1.0 / total, 0.0)


def fine_half(span, colour, coeff, weight, source, values, scaled):
    other = 1 - colour

    def body(row, low):
        near_low = low if colour == 0 else jnp.logical_not(low)
        mine = inner(coeff[colour], row)
        summed = mine * fine_sum(values[other], row, near_low)
        summed = summed + fine_sum(scaled[other], row, near_low)
        fresh = weight[colour][row] * (source[colour][row] + summed)
        put(values[colour], row, fresh)
        put(scaled[colour], row, mine * fresh)

    over_rows(span, low_rows(coeff[0].shape[1] - 2 * PAD), body)


def mid_half(span, colour, coeff, weight, source, values, scaled):
    def body(row, red):
        chosen = red if colour == 0 else jnp.logical_not(red)
        mine = inner(coeff, row)
        summed = mine * mid_sum(values, row) + mid_sum(scaled, row)
        fresh = weight[row] * (source[row] + summed)
        fresh = jnp.where(chosen, fresh, inner(values, row))
        put(values, row, fresh)
        put(scaled, row, mine * fresh)

    over_rows(span, red_lanes(coeff.shape[1] - 2 * PAD), body)


def shrink(span, rows):
    first, last = span[0] + rows, span[1] - rows
    return first - first % 2, last + last % 2


def way_down(geo, coefficient, ends, source):
    bx, wx, wy, mx, my = geo.bx, geo.wx, geo.wy, geo.mx, geo.my
    cx, cy = geo.cx, geo.cy
    lx, ly = cx // 2, cy // 2
    rows = coefficient_rows(geo)
    top = bx - COEFF_ROWS
    share = geo.bz // 4
    kept = (bx - FINE_ROWS, 2 * bx + FINE_ROWS)
    depth = kept[1] - kept[0]

    def kernel(*refs):
        coeff_in, (before, after), source_in = refs[0:3], refs[3:5], refs[5:8]
        payload, sent_low, sent_high, center, mid_coeff, mid_weight = refs[8:14]
        out_black, out_coeff, out_weight, out_source = refs[14:18]
        kr, kb, vr, vb, wr, wb, weight_r, weight_b, source_r, source_b = refs[18:28]
        diag, resid, mc, mv, mw, mid_source, mid_diag = refs[28:]
        coeff, values, scaled = (kr, kb), (vr, vb), (wr, wb)
        weight, sources = (weight_r, weight_b), (source_r, source_b)
        for ref in (kr, kb, vr, vb, wr, wb, mc, mv, mw):
            clear_pads(ref)

        lane = iota((wy, LANES), 1)
        is_own, is_after = lane < LANES // 2, lane < LANES // 2 + Z_PAIRS
        is_before = lane >= LANES - Z_PAIRS
        for index, (part, row) in enumerate(rows):
            line, shift = index // 4, index % 4 * Z_PAIRS
            own, prior, later = coeff_in[part][row], before[line], after[line]
            for colour, own_turn, turn in ((0, 0, LANES // 2), (1, LANES // 2, 0)):
                lanes = pltpu.roll(own, own_turn, 1) if own_turn else own
                after_turn = (turn - shift) % LANES
                before_turn = (turn + shift) % LANES
                near = pltpu.roll(later, after_turn, 1) if after_turn else later
                past = pltpu.roll(prior, before_turn, 1) if before_turn else prior
                lanes = jnp.where(
                    is_own,
                    lanes,
                    jnp.where(is_after, near, jnp.where(is_before, past, 0.0)),
                )
                put(coeff[colour], top + index, 0.5 * lanes)
        edge = jnp.zeros((wy, LANES), F32)
        for colour in (0, 1):
            for row in (*range(top), *range(top + len(rows), wx)):
                put(coeff[colour], row, edge)
            sources[colour][bx - SOURCE_ROWS : bx] = source_in[0][colour].astype(F32)
            sources[colour][bx : 2 * bx] = source_in[1][colour].astype(F32)
            sources[colour][2 * bx : 2 * bx + SOURCE_ROWS] = source_in[2][colour].astype(F32)

        span = (bx - SOURCE_ROWS, 2 * bx + SOURCE_ROWS)
        lower = low_rows(wy)

        def first_red(row, low):
            mine = inner(kr, row)
            total = 6.0 * mine + fine_sum(kb, row, low)
            inverse = weights(mine, total)
            diag[row] = total
            weight_r[row] = inverse
            fresh = inverse * source_r[row]
            put(vr, row, fresh)
            put(wr, row, mine * fresh)

        over_rows(span, lower, first_red)

        def black_weight(row, low):
            mine = inner(kb, row)
            total = 6.0 * mine + fine_sum(kr, row, jnp.logical_not(low))
            weight_b[row] = weights(mine, total)

        over_rows(shrink(span, 1), lower, black_weight)
        fine_half(shrink(span, 1), 1, coeff, weight, sources, values, scaled)
        fine_half(shrink(span, 2), 0, coeff, weight, sources, values, scaled)
        fine_half(shrink(span, 3), 1, coeff, weight, sources, values, scaled)

        def residual(row, low):
            mine = inner(kr, row)
            summed = mine * fine_sum(vb, row, low) + fine_sum(wb, row, low)
            resid[row] = source_r[row] + summed - diag[row] * inner(vr, row)

        over_rows(shrink(span, 4), lower, residual)
        kept_at = geo.kept_y()[0]
        strip = pl.ds(kept_at, geo.fy)
        inner_strip = pl.ds(pl.multiple_of(kept_at + PAD, 8), geo.fy)
        for row in range(depth):
            at = kept[0] + row
            out_black[row] = vb[at + 1, inner_strip, :]
            for colour in (0, 1):
                out_coeff[colour, row] = coeff[colour][at + 1, inner_strip, :]
                out_weight[colour, row] = weight[colour][at, strip, :]
                out_source[colour, row] = sources[colour][at, strip, :].astype(BF16)

        mid_span = (cx - SOURCE_ROWS // 2, 2 * cx + SOURCE_ROWS // 2)
        mid_sourced = shrink(mid_span, 2)
        blank = jnp.zeros((my, LANES), F32)
        for row in range(mx):
            if not mid_span[0] <= row < mid_span[1]:
                put(mc, row, blank)
                put(mv, row, blank)
                put(mw, row, blank)
                continue
            at = 2 * row
            diag[at] = (inner(kr, at) + inner(kr, at + 1)) + (inner(kb, at) + inner(kb, at + 1))
            total = diag[at, pl.ds(0, my, 2), :] + diag[at, pl.ds(1, my, 2), :]
            put(mc, row, 0.125 * total)
            if mid_sourced[0] <= row < mid_sourced[1]:
                resid[at] = resid[at] + resid[at + 1]
                total = resid[at, pl.ds(0, my, 2), :] + resid[at, pl.ds(1, my, 2), :]
                mid_source[row] = 0.5 * total
            else:
                mid_source[row] = blank

        def mid_red(row, red):
            mine = inner(mc, row)
            total = 6.0 * mine + mid_sum(mc, row)
            inverse = weights(mine, total)
            mid_diag[row] = total
            mid_weight[row] = inverse
            fresh = jnp.where(red, inverse * mid_source[row], 0.0)
            put(mv, row, fresh)
            put(mw, row, mine * fresh)

        over_rows(mid_span, red_lanes(my), mid_red)
        for rows_off, colour in ((1, 1), (2, 0), (3, 1)):
            mid_half(
                shrink(mid_sourced, rows_off), colour, mc, mid_weight, mid_source, mv, mw
            )
        own = (cx, 2 * cx)

        def mid_residual(row, red):
            mine = inner(mc, row)
            summed = mine * mid_sum(mv, row) + mid_sum(mw, row)
            left = mid_source[row] + summed - mid_diag[row] * inner(mv, row)
            mid_diag[row] = jnp.where(red, 0.25 * left, 0.0)

        over_rows(own, red_lanes(my), mid_residual)
        for row in range(mx):
            mid_coeff[row] = inner(mc, row)
        for row in range(cx):
            center[0, row] = inner(mv, cx + row)
            center[1, row] = mid_source[cx + row]
        sent_low[...] = center[:, 0:MID_ROWS]
        sent_high[...] = center[:, cx - MID_ROWS :]

        start = geo.own_y(cy)
        parts = []
        for cell in range(lx):
            at = cx + 2 * cell
            mid_diag[at] = mid_diag[at] + mid_diag[at + 1]
            mid_diag[at + 1] = inner(mc, at) + inner(mc, at + 1)
            halves = []
            for row in (at, at + 1):
                first = mid_diag[row, pl.ds(start, ly, 2), :]
                halves.append(first + mid_diag[row, pl.ds(start + 1, ly, 2), :])
            parts.append(jnp.concatenate(halves, axis=0))
        from_lane = iota((LANES, LANES), 0)
        to_lane = iota((LANES, LANES), 1)
        total = jnp.zeros((2 * ly, LANES), F32)
        for cell in range(lx):
            fold = (to_lane == from_lane // 2 + cell * share) & (from_lane < 2 * share)
            total = total + exact_dot(parts[cell], jnp.where(fold, 0.125, 0.0))
        payload[...] = jnp.broadcast_to(total[None], payload.shape)

    slab = shape_f32(2, MID_ROWS, my, LANES)
    middle = shape_f32(mx, my, LANES)
    both = shape_f32(2, depth, geo.fy, LANES)
    source_kept = jax.ShapeDtypeStruct((2, depth, geo.fy, LANES), BF16)
    plain = pltpu.VMEM((wx, wy, LANES), F32)
    small = pltpu.VMEM((mx, my, LANES), F32)
    return call(
        kernel,
        [
            shape_f32(geo.devices, 2 * ly, LANES),
            slab,
            slab,
            shape_f32(2, cx, my, LANES),
            middle,
            middle,
            shape_f32(depth, geo.fy, LANES),
            both,
            both,
            source_kept,
        ],
        [padded(wx, wy)] * 6 + [plain] * 6 + [padded(mx, my)] * 3 + [small] * 2,
        room=20 if geo.swap else 40,
    )(*coefficient, *ends, *source)


def low_shift(values, dim, step):
    size = values.shape[dim]
    if dim == 0:
        blank = jnp.zeros_like(values[0:1])
        if step < 0:
            return jnp.concatenate([blank, values[:-1]], axis=0)
        return jnp.concatenate([values[1:], blank], axis=0)
    turned = pltpu.roll(values, 1 if step < 0 else size - 1, dim)
    edge = 0 if step < 0 else size - 1
    return jnp.where(iota(values.shape, dim) == edge, 0.0, turned)


def low_sum(values):
    total = low_shift(values, 0, -1) + low_shift(values, 0, 1)
    for dim in (1, 2):
        total = total + low_shift(values, dim, -1) + low_shift(values, dim, 1)
    return total


def bottom_solve(rhs, half_coeff):
    diag = 6.0 * half_coeff + low_sum(half_coeff)

    def apply(values):
        summed = half_coeff * low_sum(values) + low_sum(half_coeff * values)
        return (diag * values - summed) * 0.0625

    image = apply(rhs)
    alpha = jnp.sum(rhs * rhs) / jnp.sum(rhs * image)
    rest = rhs - alpha * image
    turned = apply(rest)
    omega = jnp.sum(turned * rest) / jnp.sum(turned * turned)
    return alpha * rhs + omega * rest


def lift_bottom(geo, lows):
    bz, mx, my = geo.bz, geo.mx, geo.my
    cx, cy = geo.cx, geo.cy
    block_x, block_y = cx // 2, cy // 2
    lx, ly = geo.gx * block_x, geo.gy * block_y
    share = bz // 4
    groups = LANES // share
    columns = geo.gz * share

    def kernel(low_ref, out_ref, low_full, spread):
        lane = iota((2 * block_y, LANES), 1) // share
        for ix in range(geo.gx):
            for iy in range(geo.gy):
                for group in range(block_x):
                    for tile in range(columns // LANES):
                        total = jnp.zeros((2 * block_y, LANES), F32)
                        for part in range(groups):
                            device = (ix * geo.gy + iy) * geo.gz + tile * groups + part
                            piece = low_ref[device]
                            shift = ((part - group) * share) % LANES
                            if shift:
                                piece = pltpu.roll(piece, shift, 1)
                            total = jnp.where(lane == part, piece, total)
                        at = slice(tile * LANES, (tile + 1) * LANES)
                        to = slice(iy * block_y, (iy + 1) * block_y)
                        low_full[0, ix * block_x + group, to, at] = total[0:block_y]
                        low_full[1, ix * block_x + group, to, at] = total[block_y:]
        bottom = bottom_solve(low_full[0], low_full[1])

        target = iota((columns, LANES), 1)
        target = jnp.where(target < LANES // 2 + LANES // 4, target, target - LANES)
        wanted = (target + LANES) // 2 - LANES // 2 + lax.axis_index("gz") * share
        copy = (iota((columns, LANES), 0) == wanted).astype(F32)
        fetched = exact_dot(bottom.reshape(lx * ly, columns), copy).reshape(lx, ly, LANES)
        edge = jnp.zeros((lx, PAD, LANES), F32)
        spread[:, 0:PAD, :] = edge
        spread[:, PAD + 2 * ly :, :] = edge
        for cell in range(lx):
            spread[cell, pl.ds(PAD, ly, 2), :] = fetched[cell]
            spread[cell, pl.ds(PAD + 1, ly, 2), :] = fetched[cell]
        begin = PAD + lax.axis_index("gy") * cy - geo.own_y(cy)
        begin = PAD if geo.swap else pl.multiple_of(begin, 8)
        first_x = lax.axis_index("gx") * block_x - block_x
        for cell in range(mx // 2):
            at = jnp.clip(first_x + cell, 0, lx - 1)
            out_ref[cell] = spread[at, pl.ds(begin, my), :]

    return call(
        kernel,
        shape_f32(mx // 2, my, LANES),
        [
            pltpu.VMEM((2, lx, ly, columns), F32),
            pltpu.VMEM((lx, 2 * ly + 2 * PAD, LANES), F32),
        ],
        room=8 if geo.swap else 24,
    )(lows)


def way_up(geo, lifted_low, mids, fines):
    bx, by, bz, wy, mx, my = geo.bx, geo.by, geo.bz, geo.wy, geo.mx, geo.my
    cx = geo.cx
    depth = bx + 2 * FINE_ROWS

    def kernel(*refs):
        low_ref, left, center, right, mid_coeff, mid_weight = refs[0:6]
        fine_black, fine_coeff, fine_weight, fine_source = refs[6:10]
        out_ref = refs[10]
        mc, mv, mw, mid_source, up, source_r, source_b = refs[11:18]
        kr, kb, vr, vb, wr, wb = refs[18:]
        for ref in (mc, mv, mw, kr, kb, vr, vb, wr, wb):
            clear_pads(ref)
        mid_span = (cx - MID_ROWS, 2 * cx + MID_ROWS)
        for row in range(mx):
            put(mc, row, mid_coeff[row])
            if not mid_span[0] <= row < mid_span[1]:
                put(mv, row, jnp.zeros((my, LANES), F32))
                put(mw, row, jnp.zeros((my, LANES), F32))
                continue
            if row < cx:
                part, place = left, row - mid_span[0]
            elif row < 2 * cx:
                part, place = center, row - cx
            else:
                part, place = right, row - 2 * cx
            mine = mid_coeff[row]
            fresh = part[0, place] + jnp.where(mine > 0.0, low_ref[row // 2], 0.0)
            mid_source[row] = part[1, place]
            put(mv, row, fresh)
            put(mw, row, mine * fresh)
        for rows_off, colour in ((1, 0), (2, 1), (3, 0), (4, 1)):
            mid_half(shrink(mid_span, rows_off), colour, mc, mid_weight, mid_source, mv, mw)

        first_mid = cx - FINE_ROWS // 2
        for cell in range(depth // 2):
            line = inner(mv, first_mid + cell)
            up[cell, pl.ds(0, my, 2), :] = line
            up[cell, pl.ds(1, my, 2), :] = line
        kept_at, own_at = geo.kept_y()
        for row in range(depth):
            red, black = fine_coeff[0, row], fine_coeff[1, row]
            put(kr, row, red)
            put(kb, row, black)
            source_r[row] = fine_source[0, row].astype(F32)
            source_b[row] = fine_source[1, row].astype(F32)
            lifted = up[row // 2, pl.ds(kept_at, geo.fy), :]
            fresh = fine_black[row] + jnp.where(black > 0.0, lifted, 0.0)
            put(vb, row, fresh)
            put(wb, row, black * fresh)
        coeff, values, scaled = (kr, kb), (vr, vb), (wr, wb)
        weight = (fine_weight.at[0], fine_weight.at[1])
        source = (source_r, source_b)
        for rows_off, colour in ((1, 0), (2, 1), (3, 0), (4, 1)):
            span = shrink((0, depth), rows_off)
            fine_half(span, colour, coeff, weight, source, values, scaled)

        own = pl.multiple_of(own_at + PAD, 8)
        span = slice(FINE_ROWS + 1, FINE_ROWS + 1 + bx)
        red = vr[span, pl.ds(own, by), :]
        black = vb[span, pl.ds(own, by), :]
        even_first = even_rows((bx, by, LANES), (0, 1))
        even = jnp.where(even_first, red, black).reshape(bx * by, LANES)
        odd = jnp.where(even_first, black, red).reshape(bx * by, LANES)
        from_lane = iota((LANES, bz), 0)
        to_lane = iota((LANES, bz), 1)
        result = exact_dot(even, (to_lane == 2 * from_lane).astype(F32))
        result = result + exact_dot(odd, (to_lane == 2 * from_lane + 1).astype(F32))
        out_ref[...] = result.reshape(bx, by, bz)

    return call(
        kernel,
        shape_f32(bx, by, bz),
        [
            padded(mx, my),
            padded(mx, my),
            padded(mx, my),
            pltpu.VMEM((mx, my, LANES), F32),
            pltpu.VMEM((depth // 2, wy, LANES), F32),
        ]
        + [pltpu.VMEM((depth, geo.fy, LANES), F32)] * 2
        + [padded(depth, geo.fy)] * 6,
        room=12 if geo.swap else 40,
    )(lifted_low, *mids, *fines)


def middle_neighbours(geo, center, low, high):
    if not geo.swap:
        own = center[:, :, geo.cy : 2 * geo.cy]
        before, after = from_neighbours("gy", geo.gy, own, own)
        center = jnp.concatenate([before, own, after], axis=2)
        low, high = center[:, :MID_ROWS], center[:, geo.cx - MID_ROWS :]
    left, right = from_neighbours("gx", geo.gx, low, high)
    return left, center, right


def per_device(geo, old_slots, old_ids, coefficient):
    center_k, low_k, high_k = widen_coefficient(geo, pack_coefficient(geo, coefficient))
    left_k, right_k = from_neighbours("gx", geo.gx, low_k, high_k)
    parts = (left_k, center_k, right_k)
    last, first = pack_ends(geo, parts)
    ends = from_neighbours("gz", geo.gz, first, last)

    center_f, low_f, high_f = gather_source(geo, old_slots, old_ids)
    left_f, right_f = from_neighbours("gx", geo.gx, low_f, high_f)

    payload, low_m, high_m, center_m, mid_coeff, mid_weight, *fines = way_down(
        geo, parts, ends, (left_f, center_f, right_f)
    )
    around = middle_neighbours(geo, center_m, low_m, high_m)
    lows = lax.all_to_all(payload, ("gx", "gy", "gz"), 0, 0, tiled=True)
    lifted = lift_bottom(geo, lows)
    return way_up(geo, lifted, (*around, mid_coeff, mid_weight), fines)


def solution(mesh):
    sizes = tuple(mesh.shape[name] for name in ("gx", "gy", "gz"))

    def body(old_slots, old_ids, old_owner, coefficient):
        del old_owner
        geo = Geometry(sizes, coefficient.shape)
        return per_device(geo, old_slots, old_ids, coefficient)

    in_specs = (
        P("gx", "gy", "gz", None),
        P("gx", "gy", "gz"),
        P("gx", "gy", None),
        P("gx", "gy", "gz"),
    )
    return jax.shard_map(
        body, mesh=mesh, in_specs=in_specs, out_specs=P("gx", "gy", "gz"), check_vma=False
    )
```

```python
import jax
import jax.numpy as jnp
from jax import lax
from jax.experimental import pallas as pl
from jax.experimental.pallas import tpu as pltpu
from jax.sharding import PartitionSpec as P


BOX = 16
SOURCE_ROWS = 12
COEFF_ROWS = SOURCE_ROWS + 1
MID_ROWS = 6
FINE_ROWS = 4
Z_PAIRS = 16
LANES = 128
HIGH = lax.Precision.HIGHEST
F32 = jnp.float32
BF16 = jnp.bfloat16


def iota(shape, dim):
    return lax.broadcasted_iota(jnp.int32, shape, dim)


def exact_dot(left, right):
    return lax.dot_general(
        left, right, (((1,), (0,)), ((), ())), precision=HIGH, preferred_element_type=F32
    )


def even_rows(shape, dims):
    total = iota(shape, dims[0])
    for dim in dims[1:]:
        total = total + iota(shape, dim)
    return total % 2 == 0


def call(kernel, outs, scratch=(), room=8):
    return pl.pallas_call(
        kernel,
        out_shape=outs,
        scratch_shapes=list(scratch),
        compiler_params=pltpu.CompilerParams(vmem_limit_bytes=room * 1024 * 1024),
    )


def shape_f32(*dims):
    return jax.ShapeDtypeStruct(dims, F32)


class Geometry:
    def __init__(self, sizes, block):
        self.gx, self.gy, self.gz = sizes
        self.bx, self.by, self.bz = block
        self.swap = self.gy == 2
        self.wx = 3 * self.bx
        self.wy = (2 if self.swap else 3) * self.by
        self.cx, self.cy = self.bx // 2, self.by // 2
        self.mx, self.my = self.wx // 2, self.wy // 2
        self.low_axes = ("gx", "gz") if self.swap else ("gx", "gy", "gz")
        self.low_blocks = 1 if self.swap else self.gy
        self.low_peers = self.gx * self.low_blocks * self.gz
        self.low_y = (self.my if self.swap else self.cy) // 2
        self.fy = self.by + (8 if self.swap else 16)

    def kept_y(self):
        if self.swap:
            start = pl.multiple_of(lax.axis_index("gy") * 8, 8)
            return start, start
        return self.by - 8, 8

    def own_y(self, rows):
        if self.swap:
            return pl.multiple_of(lax.axis_index("gy") * rows, 8)
        return rows


def is_even(axis):
    return lax.axis_index(axis) % 2 == 0


def swaps(axis, count, first, second):
    def pairs(start):
        steps = [(i, i + 1) for i in range(start, count - 1, 2)]
        return steps + [(j, i) for i, j in steps]

    return (
        lax.ppermute(first, axis, pairs(0)),
        lax.ppermute(second, axis, pairs(1)),
    )


def from_neighbours(axis, count, low, high):
    even = is_even(axis)
    first, second = swaps(
        axis, count, jnp.where(even, high, low), jnp.where(even, low, high)
    )
    return jnp.where(even, second, first), jnp.where(even, first, second)


def send_starts(axis, rows, sent):
    even = is_even(axis)
    return jnp.where(even, rows - sent, 0), jnp.where(even, 0, rows - sent)


def pack_coefficient(geo, own):
    bx, by, bz = geo.bx, geo.by, geo.bz
    half = bz // 2

    def kernel(own_ref, out_ref):
        source = iota((bz, bz), 0)
        target = iota((bz, bz), 1)
        wanted = jnp.where(target < half, 2 * target, 2 * (target - half) + 1)
        split = exact_dot(own_ref[...].reshape(bx * by, bz), (source == wanted).astype(F32))
        turned = pltpu.roll(split, half, 1)
        first = even_rows((bx, by, bz), (0, 1))
        out_ref[...] = jnp.where(
            first, split.reshape(bx, by, bz), turned.reshape(bx, by, bz)
        )

    return call(kernel, shape_f32(bx, by, bz))(own)


def widen_coefficient(geo, own):
    if not geo.swap:
        low, high = from_neighbours("gy", geo.gy, own, own)
        center = jnp.concatenate([low, own, high], axis=1)
        starts = send_starts("gx", geo.bx, COEFF_ROWS)
        return center, *(lax.dynamic_slice_in_dim(center, i, COEFF_ROWS) for i in starts)
    other = lax.ppermute(own, "gy", [(0, 1), (1, 0)])

    def kernel(own_ref, other_ref, center, *sends):
        mine = geo.own_y(geo.by)
        start = pl.multiple_of(geo.by - mine, 8)
        center[:, pl.ds(mine, geo.by), :] = own_ref[...]
        center[:, pl.ds(start, geo.by), :] = other_ref[...]
        for send, at in zip(sends, send_starts("gx", geo.bx, COEFF_ROWS)):
            send[...] = center[pl.ds(at, COEFF_ROWS)]

    slab = shape_f32(COEFF_ROWS, geo.wy, geo.bz)
    return call(kernel, [shape_f32(geo.bx, geo.wy, geo.bz), slab, slab])(own, other)


def coefficient_rows(geo):
    rows = [(0, i) for i in range(COEFF_ROWS)]
    rows += [(1, i) for i in range(geo.bx)]
    return rows + [(2, i) for i in range(COEFF_ROWS)]


def window_row(parts, part, row):
    center, first, second = parts
    if part == 1:
        return center[row]
    flip = is_even("gx") if part == 0 else jnp.logical_not(is_even("gx"))
    return jnp.where(flip, second[row], first[row])


def pack_ends(geo, parts):
    rows = coefficient_rows(geo)
    lines = -(-len(rows) // 4)

    def kernel(*refs):
        given, (sent_first, sent_second) = refs[0:3], refs[3:5]
        even = is_even("gz")
        group = iota((geo.wy, LANES), 1) % (LANES // 2) // Z_PAIRS
        for line in range(lines):
            ends = jnp.zeros((geo.wy, LANES), F32)
            starts = ends
            for place, (part, row) in enumerate(rows[4 * line : 4 * line + 4]):
                value = window_row(given, part, row)
                shift = place * Z_PAIRS
                down = pltpu.roll(value, LANES - shift, 1) if shift else value
                up = pltpu.roll(value, shift, 1) if shift else value
                ends = jnp.where(group == 3 - place, down, ends)
                starts = jnp.where(group == place, up, starts)
            sent_first[line] = jnp.where(even, ends, starts)
            sent_second[line] = jnp.where(even, starts, ends)

    packed = shape_f32(lines, geo.wy, LANES)
    return call(kernel, [packed, packed])(*parts)


def pack_source(geo, slots, cells, columns):
    bx, by = geo.bx, geo.by
    count = slots.shape[0] // columns
    tiles = cells // LANES
    boxes = 2 * geo.bz // BOX
    own_boxes = geo.bz // BOX
    per_tile = LANES // BOX
    pair = BOX // 2

    def kernel(slot_ref, center, send_a, send_b, *ordered_refs):
        place = iota((count, LANES), 1)
        wanted = jnp.where(place < own_boxes + own_boxes // 2, place, place - boxes)
        wanted = (wanted + lax.axis_index("gz") * own_boxes).astype(F32)
        rows = tiles * per_tile
        keep = iota((tiles, per_tile, LANES), 2) // BOX == iota((tiles, per_tile, LANES), 1)
        inside = iota((LANES, 2 * LANES), 0) % BOX
        target = iota((LANES, 2 * LANES), 1)
        slot_of = jnp.where(inside % 2 == 0, inside // 2, inside // 2 + LANES)
        first = even_rows((bx, by, LANES), (0, 1))
        for column, ordered in enumerate(ordered_refs):
            here = slice(column * count, (column + 1) * count)
            ids = slot_ref[here, cells : cells + LANES].astype(F32)
            chosen = (ids == wanted) & (ids >= 0.0) & (place < boxes)
            chosen = jnp.where(chosen, 1.0, 0.0).T[0:boxes].astype(BF16)
            for tile in range(tiles):
                ordered[tile] = jnp.dot(
                    chosen,
                    slot_ref[here, tile * LANES : (tile + 1) * LANES],
                    preferred_element_type=F32,
                )
            total = jnp.zeros((rows, 2 * LANES), F32)
            for box in range(boxes):
                line = ordered[:, box : box + 1, :]
                line = jnp.broadcast_to(line, (tiles, per_tile, LANES))
                line = jnp.where(keep, line, 0.0).reshape(rows, LANES).astype(BF16)
                spread = (target == slot_of + box * pair).astype(F32).astype(BF16)
                total = total + jnp.dot(line, spread, preferred_element_type=F32)
            even = total[:, 0:LANES].reshape(bx, by, LANES)
            odd = total[:, LANES:].reshape(bx, by, LANES)
            span = slice(column * by, (column + 1) * by)
            center[0, :, span, :] = jnp.where(first, even, odd).astype(BF16)
            center[1, :, span, :] = jnp.where(first, odd, even).astype(BF16)
        for send, at in zip((send_a, send_b), send_starts("gx", bx, SOURCE_ROWS)):
            send[...] = center[:, pl.ds(at, SOURCE_ROWS)]

    def shape(rows):
        return jax.ShapeDtypeStruct((2, rows, columns * by, LANES), BF16)

    return call(
        kernel,
        [shape(bx), shape(SOURCE_ROWS), shape(SOURCE_ROWS)],
        [pltpu.VMEM((tiles, boxes, LANES), F32)] * columns,
        room=12,
    )(slots)


def tag_slots(slots, ids):
    capacity, cells = slots.shape

    def kernel(slot_ref, id_ref, out_ref):
        out_ref[:, 0:cells] = slot_ref[...]
        tags = jnp.broadcast_to(id_ref[...], (capacity, LANES))
        out_ref[:, cells:] = tags.astype(F32).astype(BF16)

    shape = jax.ShapeDtypeStruct((capacity, cells + LANES), BF16)
    return call(kernel, shape)(slots, ids)


def gather_source(geo, old_slots, old_ids):
    capacity, cells = old_slots.shape[2], old_slots.shape[3]
    slots, ids = old_slots.reshape(capacity, cells), old_ids.reshape(capacity, 1)
    axes = ("gy", "gz") if geo.swap else ("gz",)
    column = lax.all_gather(tag_slots(slots, ids), axes, axis=0, tiled=True)
    if geo.swap:
        return pack_source(geo, column, cells, 2)
    own = pack_source(geo, column, cells, 1)[0]
    low, high = from_neighbours("gy", geo.gy, own, own)
    center = jnp.concatenate([low, own, high], axis=2)
    starts = send_starts("gx", geo.bx, SOURCE_ROWS)
    return center, *(lax.dynamic_slice_in_dim(center, i, SOURCE_ROWS, 1) for i in starts)


PAD = 8


def padded(rows, width):
    return pltpu.VMEM((rows + 2, width + 2 * PAD, LANES), F32)


def clear_pads(ref):
    rows, width = ref.shape[0] - 2, ref.shape[1] - 2 * PAD
    ref[0] = jnp.zeros((width + 2 * PAD, LANES), F32)
    ref[rows + 1] = jnp.zeros((width + 2 * PAD, LANES), F32)
    edge = jnp.zeros((rows + 2, PAD, LANES), F32)
    ref[:, 0:PAD, :] = edge
    ref[:, PAD + width :, :] = edge


def inner(ref, row):
    return ref[row + 1, PAD : ref.shape[1] - PAD, :]


def put(ref, row, value):
    ref[row + 1, PAD : ref.shape[1] - PAD, :] = value


def across(ref, row):
    width = ref.shape[1] - 2 * PAD
    total = inner(ref, row - 1) + inner(ref, row + 1)
    total = total + ref[row + 1, PAD - 1 : PAD - 1 + width, :]
    return total + ref[row + 1, PAD + 1 : PAD + 1 + width, :]


def fine_sum(ref, row, near_low):
    here = inner(ref, row)
    low = pltpu.roll(here, 1, 1)
    high = pltpu.roll(here, LANES - 1, 1)
    return across(ref, row) + here + jnp.where(near_low, low, high)


def mid_sum(ref, row):
    here = inner(ref, row)
    return across(ref, row) + pltpu.roll(here, 1, 1) + pltpu.roll(here, LANES - 1, 1)


def over_rows(span, mask, body):
    first, last = span
    flipped = jnp.logical_not(mask)

    def step(index, carry):
        body(first + 2 * index, mask)
        body(first + 2 * index + 1, flipped)
        return carry

    lax.fori_loop(0, (last - first) // 2, step, 0, unroll=(last - first) // 2)


def low_rows(width):
    return iota((width, LANES), 0) % 2 == 0


def red_lanes(width):
    return (iota((width, LANES), 0) + iota((width, LANES), 1)) % 2 == 0


def weights(coeff_row, total):
    return jnp.where(coeff_row > 0.0, 1.0 / total, 0.0)


def fine_half(span, colour, coeff, weight, source, values, scaled):
    other = 1 - colour

    def body(row, low):
        near_low = low if colour == 0 else jnp.logical_not(low)
        mine = inner(coeff[colour], row)
        summed = mine * fine_sum(values[other], row, near_low)
        summed = summed + fine_sum(scaled[other], row, near_low)
        fresh = weight[colour][row] * (source[colour][row] + summed)
        put(values[colour], row, fresh)
        put(scaled[colour], row, mine * fresh)

    over_rows(span, low_rows(coeff[0].shape[1] - 2 * PAD), body)


def mid_half(span, colour, coeff, weight, source, values, scaled):
    def body(row, red):
        chosen = red if colour == 0 else jnp.logical_not(red)
        mine = inner(coeff, row)
        summed = mine * mid_sum(values, row) + mid_sum(scaled, row)
        fresh = weight[row] * (source[row] + summed)
        fresh = jnp.where(chosen, fresh, inner(values, row))
        put(values, row, fresh)
        put(scaled, row, mine * fresh)

    over_rows(span, red_lanes(coeff.shape[1] - 2 * PAD), body)


def shrink(span, rows):
    first, last = span[0] + rows, span[1] - rows
    return first - first % 2, last + last % 2


def way_down(geo, coefficient, ends, source):
    bx, wx, wy, mx, my = geo.bx, geo.wx, geo.wy, geo.mx, geo.my
    cx, cy = geo.cx, geo.cy
    lx, ly = cx // 2, geo.low_y
    rows = coefficient_rows(geo)
    top = bx - COEFF_ROWS
    share = geo.bz // 4
    kept = (bx - FINE_ROWS, 2 * bx + FINE_ROWS)
    depth = kept[1] - kept[0]

    def kernel(*refs):
        coeff_in, (ends_a, ends_b), source_in = refs[0:3], refs[3:5], refs[5:8]
        payload, send_a, send_b, center, mid_coeff, mid_weight = refs[8:14]
        out_black, out_coeff, out_weight, out_source = refs[14:18]
        kr, kb, vr, vb, wr, wb, weight_r, weight_b, source_r, source_b = refs[18:28]
        diag, resid, mc, mv, mw, mid_source, mid_diag = refs[28:]
        coeff, values, scaled = (kr, kb), (vr, vb), (wr, wb)
        weight, sources = (weight_r, weight_b), (source_r, source_b)
        for ref in (kr, kb, vr, vb, wr, wb, mc, mv, mw):
            clear_pads(ref)

        lane = iota((wy, LANES), 1)
        is_own, is_after = lane < LANES // 2, lane < LANES // 2 + Z_PAIRS
        is_before = lane >= LANES - Z_PAIRS
        even_z = is_even("gz")
        for index, (part, row) in enumerate(rows):
            line, shift = index // 4, index % 4 * Z_PAIRS
            own = window_row(coeff_in, part, row)
            prior = jnp.where(even_z, ends_b[line], ends_a[line])
            later = jnp.where(even_z, ends_a[line], ends_b[line])
            for colour, own_turn, turn in ((0, 0, LANES // 2), (1, LANES // 2, 0)):
                lanes = pltpu.roll(own, own_turn, 1) if own_turn else own
                after_turn = (turn - shift) % LANES
                before_turn = (turn + shift) % LANES
                near = pltpu.roll(later, after_turn, 1) if after_turn else later
                past = pltpu.roll(prior, before_turn, 1) if before_turn else prior
                lanes = jnp.where(
                    is_own,
                    lanes,
                    jnp.where(is_after, near, jnp.where(is_before, past, 0.0)),
                )
                put(coeff[colour], top + index, 0.5 * lanes)
        edge = jnp.zeros((wy, LANES), F32)
        for colour in (0, 1):
            for row in (*range(top), *range(top + len(rows), wx)):
                put(coeff[colour], row, edge)
            even_x = is_even("gx")
            after_x, before_x = 2 * bx, bx - SOURCE_ROWS
            first_at = jnp.where(even_x, after_x, before_x)
            second_at = jnp.where(even_x, before_x, after_x)
            span = pl.ds(first_at, SOURCE_ROWS)
            sources[colour][bx : 2 * bx] = source_in[0][colour].astype(F32)
            sources[colour][span] = source_in[1][colour].astype(F32)
            span = pl.ds(second_at, SOURCE_ROWS)
            sources[colour][span] = source_in[2][colour].astype(F32)

        span = (bx - SOURCE_ROWS, 2 * bx + SOURCE_ROWS)
        lower = low_rows(wy)

        def first_red(row, low):
            mine = inner(kr, row)
            total = 6.0 * mine + fine_sum(kb, row, low)
            inverse = weights(mine, total)
            diag[row] = total
            weight_r[row] = inverse
            fresh = inverse * source_r[row]
            put(vr, row, fresh)
            put(wr, row, mine * fresh)

        over_rows(span, lower, first_red)

        def black_weight(row, low):
            mine = inner(kb, row)
            total = 6.0 * mine + fine_sum(kr, row, jnp.logical_not(low))
            weight_b[row] = weights(mine, total)

        over_rows(shrink(span, 1), lower, black_weight)
        fine_half(shrink(span, 1), 1, coeff, weight, sources, values, scaled)
        fine_half(shrink(span, 2), 0, coeff, weight, sources, values, scaled)
        fine_half(shrink(span, 3), 1, coeff, weight, sources, values, scaled)

        def residual(row, low):
            mine = inner(kr, row)
            summed = mine * fine_sum(vb, row, low) + fine_sum(wb, row, low)
            resid[row] = source_r[row] + summed - diag[row] * inner(vr, row)

        over_rows(shrink(span, 4), lower, residual)
        kept_at = geo.kept_y()[0]
        strip = pl.ds(kept_at, geo.fy)
        inner_strip = pl.ds(pl.multiple_of(kept_at + PAD, 8), geo.fy)
        for row in range(depth):
            at = kept[0] + row
            out_black[row] = vb[at + 1, inner_strip, :]
            for colour in (0, 1):
                out_coeff[colour, row] = coeff[colour][at + 1, inner_strip, :]
                out_weight[colour, row] = weight[colour][at, strip, :]
                out_source[colour, row] = sources[colour][at, strip, :].astype(BF16)

        mid_span = (cx - SOURCE_ROWS // 2, 2 * cx + SOURCE_ROWS // 2)
        mid_sourced = shrink(mid_span, 2)
        blank = jnp.zeros((my, LANES), F32)
        for row in range(mx):
            if not mid_span[0] <= row < mid_span[1]:
                put(mc, row, blank)
                put(mv, row, blank)
                put(mw, row, blank)
                continue
            at = 2 * row
            diag[at] = (inner(kr, at) + inner(kr, at + 1)) + (inner(kb, at) + inner(kb, at + 1))
            total = diag[at, pl.ds(0, my, 2), :] + diag[at, pl.ds(1, my, 2), :]
            put(mc, row, 0.125 * total)
            if mid_sourced[0] <= row < mid_sourced[1]:
                resid[at] = resid[at] + resid[at + 1]
                total = resid[at, pl.ds(0, my, 2), :] + resid[at, pl.ds(1, my, 2), :]
                mid_source[row] = 0.5 * total
            else:
                mid_source[row] = blank

        def mid_red(row, red):
            mine = inner(mc, row)
            total = 6.0 * mine + mid_sum(mc, row)
            inverse = weights(mine, total)
            mid_diag[row] = total
            mid_weight[row] = inverse
            fresh = jnp.where(red, inverse * mid_source[row], 0.0)
            put(mv, row, fresh)
            put(mw, row, mine * fresh)

        over_rows(mid_span, red_lanes(my), mid_red)
        for rows_off, colour in ((1, 1), (2, 0), (3, 1)):
            mid_half(
                shrink(mid_sourced, rows_off), colour, mc, mid_weight, mid_source, mv, mw
            )
        own = (cx, 2 * cx)

        def mid_residual(row, red):
            mine = inner(mc, row)
            summed = mine * mid_sum(mv, row) + mid_sum(mw, row)
            left = mid_source[row] + summed - mid_diag[row] * inner(mv, row)
            mid_diag[row] = jnp.where(red, 0.25 * left, 0.0)

        over_rows(own, red_lanes(my), mid_residual)
        for row in range(mx):
            mid_coeff[row] = inner(mc, row)
        for row in range(cx):
            center[0, row] = inner(mv, cx + row)
            center[1, row] = mid_source[cx + row]
        for send, at in zip((send_a, send_b), send_starts("gx", cx, MID_ROWS)):
            send[...] = center[:, pl.ds(at, MID_ROWS)]

        start = 0 if geo.swap else cy
        parts = []
        for cell in range(lx):
            at = cx + 2 * cell
            mid_diag[at] = mid_diag[at] + mid_diag[at + 1]
            mid_diag[at + 1] = inner(mc, at) + inner(mc, at + 1)
            halves = []
            for row in (at, at + 1):
                first = mid_diag[row, pl.ds(start, ly, 2), :]
                halves.append(first + mid_diag[row, pl.ds(start + 1, ly, 2), :])
            parts.append(jnp.concatenate(halves, axis=0))
        from_lane = iota((LANES, LANES), 0)
        to_lane = iota((LANES, LANES), 1)
        total = jnp.zeros((2 * ly, LANES), F32)
        for cell in range(lx):
            fold = (to_lane == from_lane // 2 + cell * share) & (from_lane < 2 * share)
            total = total + exact_dot(parts[cell], jnp.where(fold, 0.125, 0.0))
        payload[...] = jnp.broadcast_to(total[None], payload.shape)

    slab = shape_f32(2, MID_ROWS, my, LANES)
    middle = shape_f32(mx, my, LANES)
    both = shape_f32(2, depth, geo.fy, LANES)
    source_kept = jax.ShapeDtypeStruct((2, depth, geo.fy, LANES), BF16)
    plain = pltpu.VMEM((wx, wy, LANES), F32)
    small = pltpu.VMEM((mx, my, LANES), F32)
    return call(
        kernel,
        [
            shape_f32(geo.low_peers, 2 * ly, LANES),
            slab,
            slab,
            shape_f32(2, cx, my, LANES),
            middle,
            middle,
            shape_f32(depth, geo.fy, LANES),
            both,
            both,
            source_kept,
        ],
        [padded(wx, wy)] * 6 + [plain] * 6 + [padded(mx, my)] * 3 + [small] * 2,
        room=20 if geo.swap else 40,
    )(*coefficient, *ends, *source)


def low_shift(values, dim, step):
    size = values.shape[dim]
    if dim == 0:
        blank = jnp.zeros_like(values[0:1])
        if step < 0:
            return jnp.concatenate([blank, values[:-1]], axis=0)
        return jnp.concatenate([values[1:], blank], axis=0)
    turned = pltpu.roll(values, 1 if step < 0 else size - 1, dim)
    edge = 0 if step < 0 else size - 1
    return jnp.where(iota(values.shape, dim) == edge, 0.0, turned)


def low_sum(values):
    total = low_shift(values, 0, -1) + low_shift(values, 0, 1)
    for dim in (1, 2):
        total = total + low_shift(values, dim, -1) + low_shift(values, dim, 1)
    return total


def bottom_solve(rhs, half_coeff):
    diag = 6.0 * half_coeff + low_sum(half_coeff)

    def apply(values):
        summed = half_coeff * low_sum(values) + low_sum(half_coeff * values)
        return (diag * values - summed) * 0.0625

    image = apply(rhs)
    alpha = jnp.sum(rhs * rhs) / jnp.sum(rhs * image)
    rest = rhs - alpha * image
    turned = apply(rest)
    omega = jnp.sum(turned * rest) / jnp.sum(turned * turned)
    return alpha * rhs + omega * rest


def lift_bottom(geo, lows):
    bz, mx, my = geo.bz, geo.mx, geo.my
    cx, cy = geo.cx, geo.cy
    block_x, block_y = cx // 2, geo.low_y
    lx, ly = geo.gx * block_x, geo.low_blocks * block_y
    share = bz // 4
    groups = LANES // share
    columns = geo.gz * share

    def kernel(low_ref, out_ref, low_full, spread):
        lane = iota((2 * block_y, LANES), 1) // share
        for ix in range(geo.gx):
            for iy in range(geo.low_blocks):
                for group in range(block_x):
                    for tile in range(columns // LANES):
                        total = jnp.zeros((2 * block_y, LANES), F32)
                        for part in range(groups):
                            device = (ix * geo.low_blocks + iy) * geo.gz + tile * groups + part
                            piece = low_ref[device]
                            shift = ((part - group) * share) % LANES
                            if shift:
                                piece = pltpu.roll(piece, shift, 1)
                            total = jnp.where(lane == part, piece, total)
                        at = slice(tile * LANES, (tile + 1) * LANES)
                        to = slice(iy * block_y, (iy + 1) * block_y)
                        low_full[0, ix * block_x + group, to, at] = total[0:block_y]
                        low_full[1, ix * block_x + group, to, at] = total[block_y:]
        bottom = bottom_solve(low_full[0], low_full[1])

        target = iota((columns, LANES), 1)
        target = jnp.where(target < LANES // 2 + LANES // 4, target, target - LANES)
        wanted = (target + LANES) // 2 - LANES // 2 + lax.axis_index("gz") * share
        copy = (iota((columns, LANES), 0) == wanted).astype(F32)
        fetched = exact_dot(bottom.reshape(lx * ly, columns), copy).reshape(lx, ly, LANES)
        edge = jnp.zeros((lx, PAD, LANES), F32)
        spread[:, 0:PAD, :] = edge
        spread[:, PAD + 2 * ly :, :] = edge
        for cell in range(lx):
            spread[cell, pl.ds(PAD, ly, 2), :] = fetched[cell]
            spread[cell, pl.ds(PAD + 1, ly, 2), :] = fetched[cell]
        begin = PAD + lax.axis_index("gy") * cy - geo.own_y(cy)
        begin = PAD if geo.swap else pl.multiple_of(begin, 8)
        first_x = lax.axis_index("gx") * block_x - block_x
        for cell in range(mx // 2):
            at = jnp.clip(first_x + cell, 0, lx - 1)
            out_ref[cell] = spread[at, pl.ds(begin, my), :]

    return call(
        kernel,
        shape_f32(mx // 2, my, LANES),
        [
            pltpu.VMEM((2, lx, ly, columns), F32),
            pltpu.VMEM((lx, 2 * ly + 2 * PAD, LANES), F32),
        ],
        room=8 if geo.swap else 24,
    )(lows)


def way_up(geo, lifted_low, mids, fines):
    bx, by, bz, wy, mx, my = geo.bx, geo.by, geo.bz, geo.wy, geo.mx, geo.my
    cx = geo.cx
    depth = bx + 2 * FINE_ROWS

    def kernel(*refs):
        low_ref, center, first, second, mid_coeff, mid_weight = refs[0:6]
        fine_black, fine_coeff, fine_weight, fine_source = refs[6:10]
        out_ref = refs[10]
        mc, mv, mw, mid_source, up, source_r, source_b = refs[11:18]
        kr, kb, vr, vb, wr, wb = refs[18:]
        for ref in (mc, mv, mw, kr, kb, vr, vb, wr, wb):
            clear_pads(ref)
        mid_span = (cx - MID_ROWS, 2 * cx + MID_ROWS)
        for row in range(mx):
            put(mc, row, mid_coeff[row])
            if not mid_span[0] <= row < mid_span[1]:
                put(mv, row, jnp.zeros((my, LANES), F32))
                put(mw, row, jnp.zeros((my, LANES), F32))
                continue
            if row < cx:
                part, place = 0, row - mid_span[0]
            elif row < 2 * cx:
                part, place = 1, row - cx
            else:
                part, place = 2, row - 2 * cx
            mine = mid_coeff[row]
            values = window_row((center.at[0], first.at[0], second.at[0]), part, place)
            fresh = values + jnp.where(mine > 0.0, low_ref[row // 2], 0.0)
            mid_source[row] = window_row(
                (center.at[1], first.at[1], second.at[1]), part, place
            )
            put(mv, row, fresh)
            put(mw, row, mine * fresh)
        for rows_off, colour in ((1, 0), (2, 1), (3, 0), (4, 1)):
            mid_half(shrink(mid_span, rows_off), colour, mc, mid_weight, mid_source, mv, mw)

        first_mid = cx - FINE_ROWS // 2
        for cell in range(depth // 2):
            line = inner(mv, first_mid + cell)
            up[cell, pl.ds(0, my, 2), :] = line
            up[cell, pl.ds(1, my, 2), :] = line
        kept_at, own_at = geo.kept_y()
        for row in range(depth):
            red, black = fine_coeff[0, row], fine_coeff[1, row]
            put(kr, row, red)
            put(kb, row, black)
            source_r[row] = fine_source[0, row].astype(F32)
            source_b[row] = fine_source[1, row].astype(F32)
            lifted = up[row // 2, pl.ds(kept_at, geo.fy), :]
            fresh = fine_black[row] + jnp.where(black > 0.0, lifted, 0.0)
            put(vb, row, fresh)
            put(wb, row, black * fresh)
        coeff, values, scaled = (kr, kb), (vr, vb), (wr, wb)
        weight = (fine_weight.at[0], fine_weight.at[1])
        source = (source_r, source_b)
        for rows_off, colour in ((1, 0), (2, 1), (3, 0), (4, 1)):
            span = shrink((0, depth), rows_off)
            fine_half(span, colour, coeff, weight, source, values, scaled)

        own = pl.multiple_of(own_at + PAD, 8)
        span = slice(FINE_ROWS + 1, FINE_ROWS + 1 + bx)
        red = vr[span, pl.ds(own, by), :]
        black = vb[span, pl.ds(own, by), :]
        even_first = even_rows((bx, by, LANES), (0, 1))
        even = jnp.where(even_first, red, black).reshape(bx * by, LANES)
        odd = jnp.where(even_first, black, red).reshape(bx * by, LANES)
        from_lane = iota((LANES, bz), 0)
        to_lane = iota((LANES, bz), 1)
        result = exact_dot(even, (to_lane == 2 * from_lane).astype(F32))
        result = result + exact_dot(odd, (to_lane == 2 * from_lane + 1).astype(F32))
        out_ref[...] = result.reshape(bx, by, bz)

    return call(
        kernel,
        shape_f32(bx, by, bz),
        [
            padded(mx, my),
            padded(mx, my),
            padded(mx, my),
            pltpu.VMEM((mx, my, LANES), F32),
            pltpu.VMEM((depth // 2, wy, LANES), F32),
        ]
        + [pltpu.VMEM((depth, geo.fy, LANES), F32)] * 2
        + [padded(depth, geo.fy)] * 6,
        room=12 if geo.swap else 40,
    )(lifted_low, *mids, *fines)


def middle_neighbours(geo, center, first, second):
    if not geo.swap:
        own = center[:, :, geo.cy : 2 * geo.cy]
        before, after = from_neighbours("gy", geo.gy, own, own)
        center = jnp.concatenate([before, own, after], axis=2)
        starts = send_starts("gx", geo.cx, MID_ROWS)
        first, second = (
            lax.dynamic_slice_in_dim(center, i, MID_ROWS, 1) for i in starts
        )
    return center, *swaps("gx", geo.gx, first, second)


def per_device(geo, old_slots, old_ids, coefficient):
    center_k, *sent_k = widen_coefficient(geo, pack_coefficient(geo, coefficient))
    parts = (center_k, *swaps("gx", geo.gx, *sent_k))
    sent_z = pack_ends(geo, parts)
    ends = swaps("gz", geo.gz, *sent_z)

    center_f, *sent_f = gather_source(geo, old_slots, old_ids)
    source = (center_f, *swaps("gx", geo.gx, *sent_f))

    payload, first_m, second_m, center_m, mid_coeff, mid_weight, *fines = way_down(
        geo, parts, ends, source
    )
    around = middle_neighbours(geo, center_m, first_m, second_m)
    lows = lax.all_to_all(payload, geo.low_axes, 0, 0, tiled=True)
    lifted = lift_bottom(geo, lows)
    return way_up(geo, lifted, (*around, mid_coeff, mid_weight), fines)


def solution(mesh):
    sizes = tuple(mesh.shape[name] for name in ("gx", "gy", "gz"))

    def body(old_slots, old_ids, old_owner, coefficient):
        del old_owner
        geo = Geometry(sizes, coefficient.shape)
        return per_device(geo, old_slots, old_ids, coefficient)

    in_specs = (
        P("gx", "gy", "gz", None),
        P("gx", "gy", "gz"),
        P("gx", "gy", None),
        P("gx", "gy", "gz"),
    )
    return jax.shard_map(
        body, mesh=mesh, in_specs=in_specs, out_specs=P("gx", "gy", "gz"), check_vma=False
    )
```

```python
import jax
import jax.numpy as jnp
from jax import lax
from jax.experimental import pallas as pl
from jax.experimental.pallas import tpu as pltpu
from jax.sharding import PartitionSpec as P


BOX = 16
SOURCE_ROWS = 12
COEFF_ROWS = SOURCE_ROWS + 1
MID_ROWS = 6
FINE_ROWS = 4
Z_PAIRS = 16
LANES = 128
HIGH = lax.Precision.HIGHEST
F32 = jnp.float32
BF16 = jnp.bfloat16
I16 = jnp.int16

ROOT_LOW, ROOT_HIGH = 0.2**0.5, 5.0**0.5
ROOT_MID = 0.5 * (ROOT_LOW + ROOT_HIGH)
ROOT_STEP = 0.5 * (ROOT_HIGH - ROOT_LOW) / 32767.0


def encode(values):
    code = jnp.floor((jnp.sqrt(values) - ROOT_MID) * (1.0 / ROOT_STEP) + 0.5)
    code = jnp.clip(code, -32767.0, 32767.0)
    return jnp.where(code == 0.0, 1.0, code)


def to_i16(code):
    return code.astype(jnp.int32).astype(I16)


def from_i16(code):
    return code.astype(jnp.int32).astype(F32)


def decode(code):
    code = from_i16(code)
    root = ROOT_MID + ROOT_STEP * code
    return jnp.where(code == 0.0, 0.0, root * root)


def iota(shape, dim):
    return lax.broadcasted_iota(jnp.int32, shape, dim)


def exact_dot(left, right):
    return lax.dot_general(
        left, right, (((1,), (0,)), ((), ())), precision=HIGH, preferred_element_type=F32
    )


def even_rows(shape, dims):
    total = iota(shape, dims[0])
    for dim in dims[1:]:
        total = total + iota(shape, dim)
    return total % 2 == 0


def call(kernel, outs, scratch=(), room=8):
    return pl.pallas_call(
        kernel,
        out_shape=outs,
        scratch_shapes=list(scratch),
        compiler_params=pltpu.CompilerParams(vmem_limit_bytes=room * 1024 * 1024),
    )


def shape_f32(*dims):
    return jax.ShapeDtypeStruct(dims, F32)


class Geometry:
    def __init__(self, sizes, block):
        self.gx, self.gy, self.gz = sizes
        self.bx, self.by, self.bz = block
        self.swap = self.gy == 2
        self.wx = 3 * self.bx
        self.wy = (2 if self.swap else 3) * self.by
        self.cx, self.cy = self.bx // 2, self.by // 2
        self.mx, self.my = self.wx // 2, self.wy // 2
        self.low_axes = ("gx", "gz") if self.swap else ("gx", "gy", "gz")
        self.low_blocks = 1 if self.swap else self.gy
        self.low_peers = self.gx * self.low_blocks * self.gz
        self.low_y = (self.my if self.swap else self.cy) // 2
        self.fy = self.by + (8 if self.swap else 16)

    def kept_y(self):
        if self.swap:
            start = pl.multiple_of(lax.axis_index("gy") * 8, 8)
            return start, start
        return self.by - 8, 8

    def own_y(self, rows):
        if self.swap:
            return pl.multiple_of(lax.axis_index("gy") * rows, 8)
        return rows


def is_even(axis):
    return lax.axis_index(axis) % 2 == 0


def swaps(axis, count, first, second):
    def pairs(start):
        steps = [(i, i + 1) for i in range(start, count - 1, 2)]
        return steps + [(j, i) for i, j in steps]

    return (
        lax.ppermute(first, axis, pairs(0)),
        lax.ppermute(second, axis, pairs(1)),
    )


def from_neighbours(axis, count, low, high):
    even = is_even(axis)
    first, second = swaps(
        axis, count, jnp.where(even, high, low), jnp.where(even, low, high)
    )
    return jnp.where(even, second, first), jnp.where(even, first, second)


def send_starts(axis, rows, sent):
    even = is_even(axis)
    return jnp.where(even, rows - sent, 0), jnp.where(even, 0, rows - sent)


def pack_coefficient(geo, own):
    bx, by, bz = geo.bx, geo.by, geo.bz
    half = bz // 2

    def kernel(own_ref, out_ref, coded_ref):
        source = iota((bz, bz), 0)
        target = iota((bz, bz), 1)
        wanted = jnp.where(target < half, 2 * target, 2 * (target - half) + 1)
        split = exact_dot(own_ref[...].reshape(bx * by, bz), (source == wanted).astype(F32))
        turned = pltpu.roll(split, half, 1)
        first = even_rows((bx, by, bz), (0, 1))
        packed = jnp.where(first, split.reshape(bx, by, bz), turned.reshape(bx, by, bz))
        out_ref[...] = packed
        coded_ref[...] = to_i16(encode(packed))

    coded = jax.ShapeDtypeStruct((bx, by, bz), I16)
    return call(kernel, [shape_f32(bx, by, bz), coded])(own)


def widen_coefficient(geo, own):
    if not geo.swap:
        low, high = from_neighbours("gy", geo.gy, own, own)
        center = jnp.concatenate([low, own, high], axis=1)
        starts = send_starts("gx", geo.bx, COEFF_ROWS)
        return center, *(lax.dynamic_slice_in_dim(center, i, COEFF_ROWS) for i in starts)
    other = lax.ppermute(own, "gy", [(0, 1), (1, 0)])

    def kernel(own_ref, other_ref, center, *sends):
        mine = geo.own_y(geo.by)
        start = pl.multiple_of(geo.by - mine, 8)
        center[:, pl.ds(mine, geo.by), :] = own_ref[...]
        center[:, pl.ds(start, geo.by), :] = other_ref[...]
        for send, at in zip(sends, send_starts("gx", geo.bx, COEFF_ROWS)):
            send[...] = center[pl.ds(at, COEFF_ROWS)]

    slab = jax.ShapeDtypeStruct((COEFF_ROWS, geo.wy, geo.bz), I16)
    whole = jax.ShapeDtypeStruct((geo.bx, geo.wy, geo.bz), I16)
    return call(kernel, [whole, slab, slab])(own, other)


def coefficient_rows(geo):
    rows = [(0, i) for i in range(COEFF_ROWS)]
    rows += [(1, i) for i in range(geo.bx)]
    return rows + [(2, i) for i in range(COEFF_ROWS)]


def window_row(parts, part, row, read=lambda value: value):
    center, first, second = parts
    if part == 1:
        return read(center[row])
    flip = is_even("gx") if part == 0 else jnp.logical_not(is_even("gx"))
    return jnp.where(flip, read(second[row]), read(first[row]))


def pack_ends(geo, parts):
    rows = coefficient_rows(geo)
    lines = -(-len(rows) // 4)

    def kernel(*refs):
        given, (sent_first, sent_second) = refs[0:3], refs[3:5]
        even = is_even("gz")
        lane = iota((geo.wy, LANES), 1)
        half = LANES // 2
        group = lane % half // Z_PAIRS
        for line in range(lines):
            ends = jnp.zeros((geo.wy, LANES), F32)
            starts = ends
            for place, (part, row) in enumerate(rows[4 * line : 4 * line + 4]):
                value = window_row(given, part, row, from_i16)
                shift = place * Z_PAIRS
                moved = pltpu.roll(value, shift, 1) if shift else value
                last = (half - Z_PAIRS + shift) % half // Z_PAIRS
                ends = jnp.where(group == last, moved, ends)
                starts = jnp.where(group == place, moved, starts)
            sent_first[line] = to_i16(jnp.where(even, ends, starts))
            sent_second[line] = to_i16(jnp.where(even, starts, ends))

    packed = jax.ShapeDtypeStruct((lines, geo.wy, LANES), I16)
    return call(kernel, [packed, packed])(*parts)


def pack_source(geo, slots, cells, columns):
    bx, by = geo.bx, geo.by
    count = slots.shape[0] // columns
    tiles = cells // LANES
    boxes = 2 * geo.bz // BOX
    own_boxes = geo.bz // BOX
    per_tile = LANES // BOX
    pair = BOX // 2

    def kernel(slot_ref, center, send_a, send_b, *ordered_refs):
        place = iota((count, LANES), 1)
        wanted = jnp.where(place < own_boxes + own_boxes // 2, place, place - boxes)
        wanted = (wanted + lax.axis_index("gz") * own_boxes).astype(F32)
        rows = tiles * per_tile
        keep = iota((tiles, per_tile, LANES), 2) // BOX == iota((tiles, per_tile, LANES), 1)
        inside = iota((2 * LANES, 2 * LANES), 0)
        target = iota((2 * LANES, 2 * LANES), 1)
        slot_of = inside // LANES * pair + inside % BOX // 2
        slot_of = slot_of + inside % 2 * LANES
        first = even_rows((bx, by, LANES), (0, 1))
        for column, ordered in enumerate(ordered_refs):
            here = slice(column * count, (column + 1) * count)
            ids = slot_ref[here, cells : cells + LANES].astype(F32)
            chosen = (ids == wanted) & (ids >= 0.0) & (place < boxes)
            chosen = jnp.where(chosen, 1.0, 0.0).T[0:boxes].astype(BF16)
            for tile in range(tiles):
                ordered[tile] = jnp.dot(
                    chosen,
                    slot_ref[here, tile * LANES : (tile + 1) * LANES],
                    preferred_element_type=F32,
                )
            total = jnp.zeros((rows, 2 * LANES), F32)
            for box in range(0, boxes, 2):
                lines = []
                for which in (box, box + 1):
                    line = ordered[:, which : which + 1, :]
                    line = jnp.broadcast_to(line, (tiles, per_tile, LANES))
                    line = jnp.where(keep, line, 0.0).reshape(rows, LANES)
                    lines.append(line.astype(BF16))
                line = jnp.concatenate(lines, axis=1)
                spread = (target == slot_of + box * pair).astype(F32).astype(BF16)
                total = total + jnp.dot(line, spread, preferred_element_type=F32)
            even = total[:, 0:LANES].reshape(bx, by, LANES)
            odd = total[:, LANES:].reshape(bx, by, LANES)
            span = slice(column * by, (column + 1) * by)
            center[0, :, span, :] = jnp.where(first, even, odd).astype(BF16)
            center[1, :, span, :] = jnp.where(first, odd, even).astype(BF16)
        for send, at in zip((send_a, send_b), send_starts("gx", bx, SOURCE_ROWS)):
            send[...] = center[:, pl.ds(at, SOURCE_ROWS)]

    def shape(rows):
        return jax.ShapeDtypeStruct((2, rows, columns * by, LANES), BF16)

    return call(
        kernel,
        [shape(bx), shape(SOURCE_ROWS), shape(SOURCE_ROWS)],
        [pltpu.VMEM((tiles, boxes, LANES), F32)] * columns,
        room=12,
    )(slots)


def tag_slots(slots, ids):
    capacity, cells = slots.shape

    def kernel(slot_ref, id_ref, out_ref):
        out_ref[:, 0:cells] = slot_ref[...]
        tags = jnp.broadcast_to(id_ref[...], (capacity, LANES))
        out_ref[:, cells:] = tags.astype(F32).astype(BF16)

    shape = jax.ShapeDtypeStruct((capacity, cells + LANES), BF16)
    return call(kernel, shape)(slots, ids)


def gather_source(geo, old_slots, old_ids):
    capacity, cells = old_slots.shape[2], old_slots.shape[3]
    slots, ids = old_slots.reshape(capacity, cells), old_ids.reshape(capacity, 1)
    axes = ("gy", "gz") if geo.swap else ("gz",)
    column = lax.all_gather(tag_slots(slots, ids), axes, axis=0, tiled=True)
    if geo.swap:
        return pack_source(geo, column, cells, 2)
    own = pack_source(geo, column, cells, 1)[0]
    low, high = from_neighbours("gy", geo.gy, own, own)
    center = jnp.concatenate([low, own, high], axis=2)
    starts = send_starts("gx", geo.bx, SOURCE_ROWS)
    return center, *(lax.dynamic_slice_in_dim(center, i, SOURCE_ROWS, 1) for i in starts)


PAD = 8


def padded(rows, width):
    return pltpu.VMEM((rows + 2, width + 2 * PAD, LANES), F32)


def clear_pads(ref):
    rows, width = ref.shape[0] - 2, ref.shape[1] - 2 * PAD
    ref[0] = jnp.zeros((width + 2 * PAD, LANES), F32)
    ref[rows + 1] = jnp.zeros((width + 2 * PAD, LANES), F32)
    edge = jnp.zeros((rows + 2, PAD, LANES), F32)
    ref[:, 0:PAD, :] = edge
    ref[:, PAD + width :, :] = edge


def inner(ref, row):
    return ref[row + 1, PAD : ref.shape[1] - PAD, :]


def put(ref, row, value):
    ref[row + 1, PAD : ref.shape[1] - PAD, :] = value


def across(ref, row):
    width = ref.shape[1] - 2 * PAD
    total = inner(ref, row - 1) + inner(ref, row + 1)
    total = total + ref[row + 1, PAD - 1 : PAD - 1 + width, :]
    return total + ref[row + 1, PAD + 1 : PAD + 1 + width, :]


def around(ref, row):
    return across(ref, row) + inner(ref, row)


def beside(first, second, colour):
    even = iota(first.shape, 0) % 2 == 0
    if colour == 1:
        even = jnp.logical_not(even)
    low = pltpu.roll(jnp.where(even, first, second), 1, 1)
    high = pltpu.roll(jnp.where(even, second, first), LANES - 1, 1)
    return jnp.where(even, low, high), jnp.where(even, high, low)


def over_pairs(span, body):
    first, last = span

    def step(index, carry):
        body(first + 2 * index)
        return carry

    lax.fori_loop(0, (last - first) // 2, step, 0, unroll=(last - first) // 2)


def over_rows(span, mask, body):
    flipped = jnp.logical_not(mask)

    def both(row):
        body(row, mask)
        body(row + 1, flipped)

    over_pairs(span, both)


def red_lanes(width):
    return (iota((width, LANES), 0) + iota((width, LANES), 1)) % 2 == 0


def weights(coeff_row, total):
    return jnp.where(coeff_row > 0.0, 1.0 / total, 0.0)


def fine_sums(row, colour, coeff, side, values, scaled):
    other = 1 - colour
    sixth = beside(inner(values[other], row), inner(values[other], row + 1), colour)
    sums = []
    for at, value in zip((row, row + 1), sixth):
        total = inner(coeff[colour], at) * around(values[other], at)
        sums.append(total + around(scaled[other], at) + side[colour][at] * value)
    return sums


def fine_half(span, colour, coeff, side, weight, source, values, scaled):
    def body(row):
        sums = fine_sums(row, colour, coeff, side, values, scaled)
        for at, summed in zip((row, row + 1), sums):
            fresh = weight[colour][at] * (source[colour][at] + summed)
            put(values[colour], at, fresh)
            put(scaled[colour], at, inner(coeff[colour], at) * fresh)

    over_pairs(span, body)


def mid_sides(ref, row):
    here = inner(ref, row)
    return pltpu.roll(here, 1, 1), pltpu.roll(here, LANES - 1, 1)


def mid_sums(row, coeff, side, values, scaled):
    below, above = mid_sides(values, row)
    total = inner(coeff, row) * across(values, row) + across(scaled, row)
    return total + side[0][row] * below + side[1][row] * above


def mid_half(span, colour, coeff, side, weight, source, values, scaled):
    def body(row, red):
        chosen = red if colour == 0 else jnp.logical_not(red)
        summed = mid_sums(row, coeff, side, values, scaled)
        fresh = weight[row] * (source[row] + summed)
        fresh = jnp.where(chosen, fresh, inner(values, row))
        put(values, row, fresh)
        put(scaled, row, inner(coeff, row) * fresh)

    over_rows(span, red_lanes(coeff.shape[1] - 2 * PAD), body)


def shrink(span, rows):
    first, last = span[0] + rows, span[1] - rows
    return first - first % 2, last + last % 2


def way_down(geo, own_coefficient, coefficient, ends, source):
    bx, wx, wy, mx, my = geo.bx, geo.wx, geo.wy, geo.mx, geo.my
    cx, cy = geo.cx, geo.cy
    lx, ly = cx // 2, geo.low_y
    rows = coefficient_rows(geo)
    top = bx - COEFF_ROWS
    share = geo.bz // 4
    kept = (bx - FINE_ROWS, 2 * bx + FINE_ROWS)
    depth = kept[1] - kept[0]

    def kernel(*refs):
        own_exact, refs = refs[0], refs[1:]
        coeff_in, (ends_a, ends_b), source_in = refs[0:3], refs[3:5], refs[5:8]
        payload, send_a, send_b, center, mid_coeff, mid_weight = refs[8:14]
        out_black, out_coeff, out_weight, out_source = refs[14:18]
        kr, kb, vr, vb, wr, wb, weight_r, weight_b, source_r, source_b = refs[18:28]
        diag, resid, side_r, side_b, mc, mv, mw = refs[28:35]
        mid_source, mid_diag, mid_below, mid_above, center_exact = refs[35:]
        side, mid_side = (side_r, side_b), (mid_below, mid_above)
        coeff, values, scaled = (kr, kb), (vr, vb), (wr, wb)
        weight, sources = (weight_r, weight_b), (source_r, source_b)
        for ref in (kr, kb, vr, vb, wr, wb, mc, mv, mw):
            clear_pads(ref)

        lane = iota((wy, LANES), 1)
        half = LANES // 2
        is_own = lane < half
        is_near = (lane % half < Z_PAIRS) | (lane % half >= half - Z_PAIRS)
        even_z = is_even("gz")
        for row in range(bx):
            center_exact[row] = decode(coeff_in[0][row])
        center_exact[:, pl.ds(geo.own_y(geo.by), geo.by), :] = own_exact[...]
        for index, (part, row) in enumerate(rows):
            line, place = divmod(index, 4)
            if part == 1:
                own = center_exact[row]
            else:
                own = window_row(coeff_in, part, row, decode)
            one, two = decode(ends_a[line]), decode(ends_b[line])
            from_after = (lane % half // Z_PAIRS == place) == even_z
            near = jnp.where(from_after, one, two)
            if place:
                near = pltpu.roll(near, LANES - place * Z_PAIRS, 1)
            near = jnp.where(is_near, near, 0.0)
            turned = pltpu.roll(jnp.where(is_own, near, own), half, 1)
            put(kr, top + index, 0.5 * jnp.where(is_own, own, turned))
            put(kb, top + index, 0.5 * jnp.where(is_own, turned, near))
        edge = jnp.zeros((wy, LANES), F32)
        for colour in (0, 1):
            for row in (*range(top), *range(top + len(rows), wx)):
                put(coeff[colour], row, edge)
            even_x = is_even("gx")
            after_x, before_x = 2 * bx, bx - SOURCE_ROWS
            first_at = jnp.where(even_x, after_x, before_x)
            second_at = jnp.where(even_x, before_x, after_x)
            span = pl.ds(first_at, SOURCE_ROWS)
            sources[colour][bx : 2 * bx] = source_in[0][colour].astype(F32)
            sources[colour][span] = source_in[1][colour].astype(F32)
            span = pl.ds(second_at, SOURCE_ROWS)
            sources[colour][span] = source_in[2][colour].astype(F32)

        span = (bx - SOURCE_ROWS, 2 * bx + SOURCE_ROWS)

        def first_red(row):
            sixth = beside(inner(kb, row), inner(kb, row + 1), 0)
            for at, value in zip((row, row + 1), sixth):
                mine = inner(kr, at)
                total = 6.0 * mine + around(kb, at) + value
                inverse = weights(mine, total)
                side_r[at] = mine + value
                diag[at] = total
                weight_r[at] = inverse
                fresh = inverse * source_r[at]
                put(vr, at, fresh)
                put(wr, at, mine * fresh)

        over_pairs(span, first_red)

        def first_black(row):
            sixth = beside(inner(kr, row), inner(kr, row + 1), 1)
            for at, value in zip((row, row + 1), sixth):
                mine = inner(kb, at)
                side_b[at] = mine + value
                weight_b[at] = weights(mine, 6.0 * mine + around(kr, at) + value)
            sums = fine_sums(row, 1, coeff, side, values, scaled)
            for at, summed in zip((row, row + 1), sums):
                fresh = weight_b[at] * (source_b[at] + summed)
                put(vb, at, fresh)
                put(wb, at, inner(kb, at) * fresh)

        over_pairs(shrink(span, 1), first_black)
        fine_half(shrink(span, 2), 0, coeff, side, weight, sources, values, scaled)
        fine_half(shrink(span, 3), 1, coeff, side, weight, sources, values, scaled)

        def residual(row):
            sums = fine_sums(row, 0, coeff, side, values, scaled)
            for at, summed in zip((row, row + 1), sums):
                resid[at] = source_r[at] + summed - diag[at] * inner(vr, at)

        over_pairs(shrink(span, 4), residual)
        kept_at = geo.kept_y()[0]
        strip = pl.ds(kept_at, geo.fy)
        inner_strip = pl.ds(pl.multiple_of(kept_at + PAD, 8), geo.fy)
        for row in range(depth):
            at = kept[0] + row
            out_black[row] = vb[at + 1, inner_strip, :]
            for colour in (0, 1):
                out_coeff[colour, row] = coeff[colour][at + 1, inner_strip, :]
                out_weight[colour, row] = weight[colour][at, strip, :]
                out_source[colour, row] = sources[colour][at, strip, :].astype(BF16)

        mid_span = (cx - SOURCE_ROWS // 2, 2 * cx + SOURCE_ROWS // 2)
        mid_sourced = shrink(mid_span, 2)
        blank = jnp.zeros((my, LANES), F32)
        for row in range(mx):
            if not mid_span[0] <= row < mid_span[1]:
                put(mc, row, blank)
                put(mv, row, blank)
                put(mw, row, blank)
                continue
            at = 2 * row
            diag[at] = (inner(kr, at) + inner(kr, at + 1)) + (inner(kb, at) + inner(kb, at + 1))
            total = diag[at, pl.ds(0, my, 2), :] + diag[at, pl.ds(1, my, 2), :]
            put(mc, row, 0.125 * total)
            if mid_sourced[0] <= row < mid_sourced[1]:
                resid[at] = resid[at] + resid[at + 1]
                total = resid[at, pl.ds(0, my, 2), :] + resid[at, pl.ds(1, my, 2), :]
                mid_source[row] = 0.5 * total
            else:
                mid_source[row] = blank

        def mid_red(row, red):
            mine = inner(mc, row)
            below, above = mid_sides(mc, row)
            mid_below[row] = mine + below
            mid_above[row] = mine + above
            total = 6.0 * mine + across(mc, row) + below + above
            inverse = weights(mine, total)
            mid_diag[row] = total
            mid_weight[row] = inverse
            fresh = jnp.where(red, inverse * mid_source[row], 0.0)
            put(mv, row, fresh)
            put(mw, row, mine * fresh)

        over_rows(mid_span, red_lanes(my), mid_red)
        for rows_off, colour in ((1, 1), (2, 0), (3, 1)):
            part = shrink(mid_sourced, rows_off)
            mid_half(part, colour, mc, mid_side, mid_weight, mid_source, mv, mw)
        own = (cx, 2 * cx)

        def mid_residual(row, red):
            summed = mid_sums(row, mc, mid_side, mv, mw)
            left = mid_source[row] + summed - mid_diag[row] * inner(mv, row)
            mid_diag[row] = jnp.where(red, 0.25 * left, 0.0)

        over_rows(own, red_lanes(my), mid_residual)
        for row in range(mx):
            mid_coeff[row] = inner(mc, row)
        for row in range(cx):
            center[0, row] = inner(mv, cx + row)
            center[1, row] = mid_source[cx + row]
        for send, at in zip((send_a, send_b), send_starts("gx", cx, MID_ROWS)):
            send[...] = center[:, pl.ds(at, MID_ROWS)]

        start = 0 if geo.swap else cy
        parts = []
        for cell in range(lx):
            at = cx + 2 * cell
            mid_diag[at] = mid_diag[at] + mid_diag[at + 1]
            mid_diag[at + 1] = inner(mc, at) + inner(mc, at + 1)
            halves = []
            for row in (at, at + 1):
                first = mid_diag[row, pl.ds(start, ly, 2), :]
                halves.append(first + mid_diag[row, pl.ds(start + 1, ly, 2), :])
            parts.append(jnp.concatenate(halves, axis=0))
        from_lane = iota((LANES, LANES), 0)
        to_lane = iota((LANES, LANES), 1)
        total = jnp.zeros((2 * ly, LANES), F32)
        for cell in range(lx):
            fold = (to_lane == from_lane // 2 + cell * share) & (from_lane < 2 * share)
            total = total + exact_dot(parts[cell], jnp.where(fold, 0.125, 0.0))
        payload[...] = jnp.broadcast_to(total[None], payload.shape)

    slab = shape_f32(2, MID_ROWS, my, LANES)
    middle = shape_f32(mx, my, LANES)
    both = shape_f32(2, depth, geo.fy, LANES)
    source_kept = jax.ShapeDtypeStruct((2, depth, geo.fy, LANES), BF16)
    plain = pltpu.VMEM((wx, wy, LANES), F32)
    small = pltpu.VMEM((mx, my, LANES), F32)
    return call(
        kernel,
        [
            shape_f32(geo.low_peers, 2 * ly, LANES),
            slab,
            slab,
            shape_f32(2, cx, my, LANES),
            middle,
            middle,
            shape_f32(depth, geo.fy, LANES),
            both,
            both,
            source_kept,
        ],
        [padded(wx, wy)] * 6 + [plain] * 8 + [padded(mx, my)] * 3 + [small] * 4
        + [pltpu.VMEM((bx, wy, LANES), F32)],
        room=20 if geo.swap else 40,
    )(own_coefficient, *coefficient, *ends, *source)


def low_shift(values, dim, step):
    size = values.shape[dim]
    if dim == 0:
        blank = jnp.zeros_like(values[0:1])
        if step < 0:
            return jnp.concatenate([blank, values[:-1]], axis=0)
        return jnp.concatenate([values[1:], blank], axis=0)
    turned = pltpu.roll(values, 1 if step < 0 else size - 1, dim)
    edge = 0 if step < 0 else size - 1
    return jnp.where(iota(values.shape, dim) == edge, 0.0, turned)


def low_sum(values):
    total = low_shift(values, 0, -1) + low_shift(values, 0, 1)
    for dim in (1, 2):
        total = total + low_shift(values, dim, -1) + low_shift(values, dim, 1)
    return total


def bottom_solve(rhs, half_coeff):
    diag = 6.0 * half_coeff + low_sum(half_coeff)

    def apply(values):
        summed = half_coeff * low_sum(values) + low_sum(half_coeff * values)
        return (diag * values - summed) * 0.0625

    image = apply(rhs)
    alpha = jnp.sum(rhs * rhs) / jnp.sum(rhs * image)
    rest = rhs - alpha * image
    turned = apply(rest)
    omega = jnp.sum(turned * rest) / jnp.sum(turned * turned)
    return alpha * rhs + omega * rest


def lift_bottom(geo, lows):
    bz, mx, my = geo.bz, geo.mx, geo.my
    cx, cy = geo.cx, geo.cy
    block_x, block_y = cx // 2, geo.low_y
    lx, ly = geo.gx * block_x, geo.low_blocks * block_y
    share = bz // 4
    groups = LANES // share
    columns = geo.gz * share

    def kernel(low_ref, out_ref, low_full, spread):
        lane = iota((2 * block_y, LANES), 1) // share
        for ix in range(geo.gx):
            for iy in range(geo.low_blocks):
                for group in range(block_x):
                    for tile in range(columns // LANES):
                        total = jnp.zeros((2 * block_y, LANES), F32)
                        for part in range(groups):
                            device = (ix * geo.low_blocks + iy) * geo.gz + tile * groups + part
                            piece = low_ref[device]
                            shift = ((part - group) * share) % LANES
                            if shift:
                                piece = pltpu.roll(piece, shift, 1)
                            total = jnp.where(lane == part, piece, total)
                        at = slice(tile * LANES, (tile + 1) * LANES)
                        to = slice(iy * block_y, (iy + 1) * block_y)
                        low_full[0, ix * block_x + group, to, at] = total[0:block_y]
                        low_full[1, ix * block_x + group, to, at] = total[block_y:]
        bottom = bottom_solve(low_full[0], low_full[1])

        target = iota((columns, LANES), 1)
        target = jnp.where(target < LANES // 2 + LANES // 4, target, target - LANES)
        wanted = (target + LANES) // 2 - LANES // 2 + lax.axis_index("gz") * share
        copy = (iota((columns, LANES), 0) == wanted).astype(F32)
        fetched = exact_dot(bottom.reshape(lx * ly, columns), copy).reshape(lx, ly, LANES)
        edge = jnp.zeros((lx, PAD, LANES), F32)
        spread[:, 0:PAD, :] = edge
        spread[:, PAD + 2 * ly :, :] = edge
        for cell in range(lx):
            spread[cell, pl.ds(PAD, ly, 2), :] = fetched[cell]
            spread[cell, pl.ds(PAD + 1, ly, 2), :] = fetched[cell]
        begin = PAD + lax.axis_index("gy") * cy - geo.own_y(cy)
        begin = PAD if geo.swap else pl.multiple_of(begin, 8)
        first_x = lax.axis_index("gx") * block_x - block_x
        for cell in range(mx // 2):
            at = jnp.clip(first_x + cell, 0, lx - 1)
            out_ref[cell] = spread[at, pl.ds(begin, my), :]

    return call(
        kernel,
        shape_f32(mx // 2, my, LANES),
        [
            pltpu.VMEM((2, lx, ly, columns), F32),
            pltpu.VMEM((lx, 2 * ly + 2 * PAD, LANES), F32),
        ],
        room=8 if geo.swap else 24,
    )(lows)


def way_up(geo, lifted_low, mids, fines):
    bx, by, bz, wy, mx, my = geo.bx, geo.by, geo.bz, geo.wy, geo.mx, geo.my
    cx = geo.cx
    depth = bx + 2 * FINE_ROWS

    def kernel(*refs):
        low_ref, center, first, second, mid_coeff, mid_weight = refs[0:6]
        fine_black, fine_coeff, fine_weight, fine_source = refs[6:10]
        out_ref = refs[10]
        mc, mv, mw, mid_source, mid_below, mid_above, up = refs[11:18]
        source_r, source_b, side_r, side_b = refs[18:22]
        kr, kb, vr, vb, wr, wb = refs[22:]
        side, mid_side = (side_r, side_b), (mid_below, mid_above)
        for ref in (mc, mv, mw, kr, kb, vr, vb, wr, wb):
            clear_pads(ref)
        mid_span = (cx - MID_ROWS, 2 * cx + MID_ROWS)
        for row in range(mx):
            put(mc, row, mid_coeff[row])
            if not mid_span[0] <= row < mid_span[1]:
                put(mv, row, jnp.zeros((my, LANES), F32))
                put(mw, row, jnp.zeros((my, LANES), F32))
                continue
            if row < cx:
                part, place = 0, row - mid_span[0]
            elif row < 2 * cx:
                part, place = 1, row - cx
            else:
                part, place = 2, row - 2 * cx
            mine = mid_coeff[row]
            values = window_row((center.at[0], first.at[0], second.at[0]), part, place)
            fresh = values + jnp.where(mine > 0.0, low_ref[row // 2], 0.0)
            mid_source[row] = window_row(
                (center.at[1], first.at[1], second.at[1]), part, place
            )
            put(mv, row, fresh)
            put(mw, row, mine * fresh)
            below, above = mid_sides(mc, row)
            mid_below[row] = mine + below
            mid_above[row] = mine + above
        for rows_off, colour in ((1, 0), (2, 1), (3, 0), (4, 1)):
            part = shrink(mid_span, rows_off)
            mid_half(part, colour, mc, mid_side, mid_weight, mid_source, mv, mw)

        first_mid = cx - FINE_ROWS // 2
        for cell in range(depth // 2):
            line = inner(mv, first_mid + cell)
            up[cell, pl.ds(0, my, 2), :] = line
            up[cell, pl.ds(1, my, 2), :] = line
        kept_at, own_at = geo.kept_y()
        for row in range(depth):
            red, black = fine_coeff[0, row], fine_coeff[1, row]
            put(kr, row, red)
            put(kb, row, black)
            source_r[row] = fine_source[0, row].astype(F32)
            source_b[row] = fine_source[1, row].astype(F32)
            lifted = up[row // 2, pl.ds(kept_at, geo.fy), :]
            fresh = fine_black[row] + jnp.where(black > 0.0, lifted, 0.0)
            put(vb, row, fresh)
            put(wb, row, black * fresh)
        for row in range(0, depth, 2):
            for colour, mine, other in ((0, kr, kb), (1, kb, kr)):
                sixth = beside(inner(other, row), inner(other, row + 1), colour)
                side[colour][row] = inner(mine, row) + sixth[0]
                side[colour][row + 1] = inner(mine, row + 1) + sixth[1]
        coeff, values, scaled = (kr, kb), (vr, vb), (wr, wb)
        weight = (fine_weight.at[0], fine_weight.at[1])
        source = (source_r, source_b)
        for rows_off, colour in ((1, 0), (2, 1), (3, 0), (4, 1)):
            span = shrink((0, depth), rows_off)
            fine_half(span, colour, coeff, side, weight, source, values, scaled)

        own = pl.multiple_of(own_at + PAD, 8)
        span = slice(FINE_ROWS + 1, FINE_ROWS + 1 + bx)
        red = vr[span, pl.ds(own, by), :]
        black = vb[span, pl.ds(own, by), :]
        even_first = even_rows((bx, by, LANES), (0, 1))
        even = jnp.where(even_first, red, black).reshape(bx * by, LANES)
        odd = jnp.where(even_first, black, red).reshape(bx * by, LANES)
        from_lane = iota((LANES, bz), 0)
        to_lane = iota((LANES, bz), 1)
        result = exact_dot(even, (to_lane == 2 * from_lane).astype(F32))
        result = result + exact_dot(odd, (to_lane == 2 * from_lane + 1).astype(F32))
        out_ref[...] = result.reshape(bx, by, bz)

    return call(
        kernel,
        shape_f32(bx, by, bz),
        [
            padded(mx, my),
            padded(mx, my),
            padded(mx, my),
            pltpu.VMEM((mx, my, LANES), F32),
            pltpu.VMEM((mx, my, LANES), F32),
            pltpu.VMEM((mx, my, LANES), F32),
            pltpu.VMEM((depth // 2, wy, LANES), F32),
        ]
        + [pltpu.VMEM((depth, geo.fy, LANES), F32)] * 4
        + [padded(depth, geo.fy)] * 6,
        room=12 if geo.swap else 40,
    )(lifted_low, *mids, *fines)


def middle_neighbours(geo, center, first, second):
    if not geo.swap:
        own = center[:, :, geo.cy : 2 * geo.cy]
        before, after = from_neighbours("gy", geo.gy, own, own)
        center = jnp.concatenate([before, own, after], axis=2)
        starts = send_starts("gx", geo.cx, MID_ROWS)
        first, second = (
            lax.dynamic_slice_in_dim(center, i, MID_ROWS, 1) for i in starts
        )
    return center, *swaps("gx", geo.gx, first, second)


def per_device(geo, old_slots, old_ids, coefficient):
    own_k, coded_k = pack_coefficient(geo, coefficient)
    center_k, *sent_k = widen_coefficient(geo, coded_k)
    parts = (center_k, *swaps("gx", geo.gx, *sent_k))
    sent_z = pack_ends(geo, parts)
    ends = swaps("gz", geo.gz, *sent_z)

    center_f, *sent_f = gather_source(geo, old_slots, old_ids)
    source = (center_f, *swaps("gx", geo.gx, *sent_f))

    payload, first_m, second_m, center_m, mid_coeff, mid_weight, *fines = way_down(
        geo, own_k, parts, ends, source
    )
    around = middle_neighbours(geo, center_m, first_m, second_m)
    lows = lax.all_to_all(payload, geo.low_axes, 0, 0, tiled=True)
    lifted = lift_bottom(geo, lows)
    return way_up(geo, lifted, (*around, mid_coeff, mid_weight), fines)


def solution(mesh):
    sizes = tuple(mesh.shape[name] for name in ("gx", "gy", "gz"))

    def body(old_slots, old_ids, old_owner, coefficient):
        del old_owner
        geo = Geometry(sizes, coefficient.shape)
        return per_device(geo, old_slots, old_ids, coefficient)

    in_specs = (
        P("gx", "gy", "gz", None),
        P("gx", "gy", "gz"),
        P("gx", "gy", None),
        P("gx", "gy", "gz"),
    )
    return jax.shard_map(
        body, mesh=mesh, in_specs=in_specs, out_specs=P("gx", "gy", "gz"), check_vma=False
    )
```
